512 devices in a mesh: space: 128 (over z, x, core), rad: 4 (over y).
Axes of the slice: x: 4, y: 4, z: 16, core: 2. Of those that a mesh axis runs over, the one named last changes fastest.
Arguments:
- cell_bin: int32 [8388608], P(('space', 'rad')), may hold values from 0 to 255
- cell_fields: float32 [3, 8388608], P(None, ('space', 'rad')), may hold values from 0.0005 to 0.005
- tile_halo: int32 [65536], P(('space', 'rad')), may hold values from 0 to 4095, as said below
- halo_owner: int32 [4096], replicated, may hold values from 0 to 127, as said below
Outputs:
- enclosed_mass: float32 [4096, 256], P('space', 'rad')
- enclosed_volume: float32 [4096, 256], P('space', 'rad')
- cumulative_entropy: float32 [4096, 256], P('space', 'rad')
- circular_velocity: float32 [4096, 256], P('space', 'rad')
The draws below stay inside these ranges and needn't reach their ends.
Inputs may be any that keep to these rules, and one draw needn't show every extreme that they name: `tile_halo`: the tiles of one device are in nondecreasing halo order; they go to exactly 64 owners, 2 tiles to each; the tiles of one device with one owner hold at most 1 distinct halos, and on every device some owner receives exactly 1. `halo_owner`: each index of space owns 32 consecutive halo ids.
All inputs are finite; a program needn't handle non-finite values.
Results may differ from the reference program's by a relative error of at most 0.000067.
Values sent between devices are 32-bit elements; how exact they have to be, the bound alone decides.
A program may use at most 64 MiB of HBM per device.

```python
import math
import jax
import jax.numpy as jnp

TILE = 128
BINS = 256
HALO_DEV = 32
HALOS = 4096
CAP = 2
HCAP = 1
DESTS = 64
CELLS = 8388608
N_SPACE = 128
N_RAD = 4


def layout(key):
    block_perm = jax.random.permutation(jax.random.fold_in(key, 11), N_SPACE).astype(jnp.int32)
    owner = jnp.repeat(block_perm, HALO_DEV)
    inverse = jnp.argsort(block_perm).astype(jnp.int32)

    def one_device(dkey):
        first, second, third, fourth = jax.random.split(dkey, 4)
        targets = jax.random.permutation(first, N_SPACE)[:DESTS].astype(jnp.int32)
        counts = jax.random.randint(second, (DESTS,), 1, HCAP + 1).at[0].set(HCAP)
        chosen = jax.vmap(lambda k: jax.random.permutation(k, HALO_DEV)[:HCAP])(jax.random.split(third, DESTS))
        extra = jax.random.randint(fourth, (DESTS, CAP), 0, HCAP) % counts[:, None]
        column = jnp.arange(CAP, dtype=jnp.int32)[None, :]
        slot_index = jnp.where(column < counts[:, None], column, extra)
        halo_local = jnp.take_along_axis(chosen, slot_index, axis=1)
        halos = inverse[targets][:, None] * HALO_DEV + halo_local
        return jnp.sort(halos.reshape(-1)).astype(jnp.int32)
    device_keys = jax.random.split(jax.random.fold_in(key, 12), N_SPACE * N_RAD)
    tiles = jax.vmap(one_device)(device_keys).reshape(-1)
    return (owner, tiles)


def draw_tile_halo(key, part):
    return layout(key)[1]


def draw_halo_owner(key, part):
    return layout(key)[0]


def plant(array, stream_key, smallest, largest):
    shape = array.shape
    spot = [jax.random.randint(jax.random.fold_in(stream_key, axis), (), 0, shape[axis]) for axis in range(len(shape))]
    array = array.at[tuple(spot)].set(smallest)
    longest = shape.index(max(shape))
    spot[longest] = (spot[longest] + 1) % shape[longest]
    return array.at[tuple(spot)].set(largest)


def block_levels(key, extent, shards, low, high):
    loudness = 1.0
    for dim, blocks in shards:
        steps = jax.random.uniform(jax.random.fold_in(jax.random.fold_in(key, 6), dim), (blocks,), jnp.float32, low / len(shards), high / len(shards))
        loudness = loudness * jnp.repeat(jnp.exp(steps), extent[dim] // blocks).reshape((-1,) + (1,) * (len(extent) - 1 - dim))
    return loudness


def setup_inputs(seed: int = 0) -> dict:
    key_list = jax.random.split(jax.random.key(seed), 5)
    return {
        "cell_bin": plant(jax.random.randint(key_list[0], (CELLS,), 0, BINS), jax.random.fold_in(key_list[0], 1), 0, BINS - 1).astype(jnp.int32),
        "cell_fields": jnp.clip(jnp.exp(math.log(0.005) - 2.30258502 * jax.random.uniform(key_list[1], (3, CELLS), jnp.float32) ** block_levels(key_list[1], (3, CELLS), ((1, 512),), -0.2, 0.2)), 0.0005, 0.005),
        "tile_halo": draw_tile_halo(jax.random.fold_in(key_list[4], 71), 0),
        "halo_owner": draw_halo_owner(jax.random.fold_in(key_list[4], 71), 0),
    }


log_inner = -2.302585092994046

def reference(cell_bin, cell_fields, tile_halo, halo_owner):
    cell_halo = jnp.repeat(tile_halo, TILE)
    segment = cell_halo * BINS + cell_bin
    binned = jax.ops.segment_sum(cell_fields.T, segment, num_segments=HALOS * BINS)
    binned = binned.reshape(HALOS, BINS, 3)
    running = jnp.cumsum(binned, axis=1)
    ranking = jnp.argsort(halo_owner, stable=True)
    running = running[ranking]
    position = (jnp.arange(BINS) + 1).astype(jnp.float32)
    radius = jnp.exp(log_inner + position * (-log_inner / BINS))
    enclosed = running[:, :, 0]
    velocity = jnp.sqrt(enclosed / radius[None, :])
    return (enclosed, running[:, :, 1], running[:, :, 2], velocity)
```

```python
import functools

import jax
import jax.numpy as jnp
from jax import lax
from jax.experimental import pallas as pl
from jax.experimental.pallas import tpu as pltpu
from jax.sharding import PartitionSpec as P

MESH = pl.DeviceIdType.MESH
F32 = jnp.float32
BF16 = jnp.bfloat16
TILE = 128
BINS = 256
QUARTER = 64
HALO_DEV = 32
log_inner = -2.302585092994046


def split3(v):
    high = v.astype(BF16)
    rest = v - high.astype(F32)
    mid = rest.astype(BF16)
    low = (rest - mid.astype(F32)).astype(BF16)
    return high, mid, low


def iota(shape, dim):
    return lax.broadcasted_iota(jnp.int32, shape, dim)


def nt(a, b):
    return lax.dot_general(a, b, (((1,), (1,)), ((), ())), preferred_element_type=F32)


def bin_piece(k, bin_ref, fld_ref):
    label = jnp.concatenate([bin_ref[pl.ds(2 * k, 1), :], bin_ref[pl.ds(2 * k + 1, 1), :]], axis=1)
    low = label & (QUARTER - 1)
    high = lax.shift_right_logical(label, 6)
    v = fld_ref[:, pl.ds(pl.multiple_of(2 * TILE * k, 2 * TILE), 2 * TILE)]
    pad = jnp.zeros((1, 2 * TILE), F32)
    v8 = jnp.concatenate([v, pad, v, pad], axis=0)
    row = iota((8, 2 * TILE), 0)
    parts = [[], [], []]
    bases = []
    for t in range(2):
        quarter = 2 * t + lax.shift_right_logical(row, 2)
        own = jnp.where(high == quarter, v8, 0.0)
        for s, part in enumerate(split3(own)):
            parts[s].append(part)
        bases.append(jnp.sum(jnp.where(high < quarter, v8, 0.0), axis=1, keepdims=True))
    lhs = jnp.concatenate(parts[0] + parts[1] + parts[2], axis=0)
    below = jnp.where(low <= iota((QUARTER, 2 * TILE), 0), 1.0, 0.0).astype(BF16)
    below = jnp.concatenate([below, below], axis=0)
    out = nt(lhs, below)
    out = out[0:16] + out[16:32] + out[32:48]
    return out + jnp.concatenate(bases, axis=0)


def kernel(na, nj, ny, halo_ref, owner_ref, bin_ref, fld_ref, mass_ref, vol_ref, ent_ref, vel_ref,
           pieces, code_v, code_s, send, recv, dense, got, code_sem, send1, recv1, send2, recv2):
    owners = na * nj
    count = owners // 2
    pairs = na // 2
    group = nj * ny
    rows = 3 * pairs + 1
    space = lax.axis_index("space")
    y = lax.axis_index("rad")
    a = space // nj
    j = space % nj
    me = j * ny + y

    barrier = pltpu.get_barrier_semaphore()

    def greet(i, carry):
        t = lax.rem(me + i, group)
        pl.semaphore_signal(barrier, inc=1, device_id=(a * nj + t // ny, lax.rem(t, ny)), device_id_type=MESH)
        return carry

    for i in range(1, na):
        pl.semaphore_signal(barrier, inc=1, device_id=(lax.rem(a + i, na) * nj + j, y), device_id_type=MESH)
    lax.fori_loop(1, group, greet, 0)

    lane = iota((8, owners), 1)

    def note(k, codes):
        halo = halo_ref[2 * k]
        code = 1 + HALO_DEV * k + (halo & (HALO_DEV - 1))
        return jnp.where(lane == owner_ref[halo], code, codes)

    code_v[...] = lax.fori_loop(0, count, note, jnp.zeros((8, owners), jnp.int32), unroll=min(8, count))
    noting = pltpu.make_async_copy(code_v, code_s, code_sem)
    noting.start()

    def one_piece(k, carry):
        pieces[k] = bin_piece(k, bin_ref, fld_ref)
        return carry

    lax.fori_loop(0, count, one_piece, 0, unroll=min(4, count))
    noting.wait()
    pl.semaphore_wait(barrier, group - 1 + na - 1)

    lane128 = iota((1, 128), 1)
    left = iota((16, 128), 1) < QUARTER
    tag = 128 // na

    def outbound(dj, dy):
        t = dj * ny + dy
        return pltpu.make_async_remote_copy(
            src_ref=send.at[t], dst_ref=recv.at[me], send_sem=send1.at[t], recv_sem=recv1.at[me],
            device_id=(a * nj + dj, dy), device_id_type=MESH)

    def assemble(i, carry):
        dj = lax.rem(j + 1 + i, nj)
        labels = jnp.zeros((1, 128), F32)
        for p in range(pairs):
            codes = [code_s[0, 2 * p * nj + dj], code_s[0, (2 * p + 1) * nj + dj]]
            held = [pieces[lax.shift_right_logical(jnp.maximum(c - 1, 0), 5)] for c in codes]
            there = [jnp.where(c > 0, 1, 0) for c in codes]
            both = jnp.where(left, held[0], held[1])
            both = jnp.where(jnp.where(left, there[0], there[1]) > 0, both, 0.0)
            for par in range(2):
                rank = jnp.where(codes[par] > 0, (codes[par] - 1) & (HALO_DEV - 1), -1).astype(F32)
                labels = jnp.where(lane128 // tag == 2 * p + par, rank, labels)
            for q in range(ny):
                send[dj * ny + q, 3 * p:3 * p + 3, :] = both[4 * q:4 * q + 3]
        for q in range(ny):
            send[dj * ny + q, rows - 1:rows, :] = labels
        for dy in range(ny):
            @pl.when(jnp.logical_or(dj != j, dy != y))
            def _():
                outbound(dj, dy).start()
        return carry

    lax.fori_loop(0, nj, assemble, 0)
    recv[me] = send[me]

    def inbound(t):
        return pltpu.make_async_remote_copy(
            src_ref=send.at[t], dst_ref=recv.at[t], send_sem=send1.at[t], recv_sem=recv1.at[t],
            device_id=(a * nj + t // ny, lax.rem(t, ny)), device_id_type=MESH)

    def arrive(i, carry):
        inbound(lax.rem(me + group - i, group)).wait_recv()
        return carry

    lax.fori_loop(1, group, arrive, 0)

    labels = recv[:, rows - 1, :].astype(BF16)
    labels = jnp.concatenate([labels] * 3, axis=0)
    spread = jnp.where(iota((na * HALO_DEV, 128), 1) == tag * (iota((na * HALO_DEV, 128), 0) // HALO_DEV), 1.0, 0.0).astype(BF16)
    spread = nt(spread, labels)
    wanted = (iota(spread.shape, 0) & (HALO_DEV - 1)).astype(F32)
    chosen = jnp.where(spread == wanted, 1.0, 0.0).astype(BF16)

    def onward(d):
        return pltpu.make_async_remote_copy(
            src_ref=dense.at[d], dst_ref=got.at[a], send_sem=send2.at[d], recv_sem=recv2.at[a],
            device_id=(d * nj + j, y), device_id_type=MESH)

    for p in range(pairs):
        columns = [jnp.concatenate(split3(recv[:, 3 * p + f, :]), axis=0) for f in range(3)]
        total = jnp.dot(chosen[2 * HALO_DEV * p:2 * HALO_DEV * (p + 1)], jnp.concatenate(columns, axis=1),
                        preferred_element_type=F32)
        for par in range(2):
            d = 2 * p + par
            for f in range(3):
                top = total[32 * par:32 * par + 16, 128 * f:128 * f + 128]
                bottom = total[32 * par + 16:32 * par + 32, 128 * f:128 * f + 128]
                if par == 0:
                    merged = jnp.where(left, top, pltpu.roll(bottom, QUARTER, 1))
                else:
                    merged = jnp.where(left, pltpu.roll(top, QUARTER, 1), bottom)
                dense[d, :, 128 * f:128 * f + 128] = merged

            @pl.when(d != a)
            def _():
                onward(d).start()

    total = dense[a]

    for i in range(1, na):
        t = lax.rem(a + i, na)
        pltpu.make_async_remote_copy(
            src_ref=dense.at[t], dst_ref=got.at[t], send_sem=send2.at[t], recv_sem=recv2.at[t],
            device_id=(t * nj + j, y), device_id_type=MESH).wait_recv()
        total = total + got[t]

    bins = (y * QUARTER + 1 + iota((16, QUARTER), 1)).astype(F32)
    radius = jnp.exp(log_inner + bins * (-log_inner / BINS))
    for f, ref in enumerate((mass_ref, vol_ref, ent_ref)):
        block = total[:, 128 * f:128 * f + 128]
        for half, part in enumerate((block, pltpu.roll(block, QUARTER, 1))):
            part = part[:, :QUARTER]
            ref[16 * half:16 * half + 16, :] = part
            if f == 0:
                vel_ref[16 * half:16 * half + 16, :] = jnp.sqrt(part / radius)

    def sent(i, carry):
        inbound(lax.rem(me + i, group)).wait_send()
        return carry

    lax.fori_loop(1, group, sent, 0)
    for i in range(1, na):
        onward(lax.rem(a + i, na)).wait_send()


def solution(mesh):
    spaces, ny = mesh.shape["space"], mesh.shape["rad"]
    na = 8 if spaces == 128 else 2
    nj = spaces // na
    group, rows = nj * ny, 3 * (na // 2) + 1

    def body(cell_bin, cell_fields, tile_halo, halo_owner):
        smem = pl.BlockSpec(memory_space=pltpu.SMEM)
        vmem = pl.BlockSpec(memory_space=pltpu.VMEM)
        dma = pltpu.SemaphoreType.DMA
        out = jax.ShapeDtypeStruct((HALO_DEV, QUARTER), F32)
        return pl.pallas_call(
            functools.partial(kernel, na, nj, ny),
            out_shape=(out,) * 4,
            in_specs=[smem, smem, vmem, vmem],
            out_specs=(vmem,) * 4,
            scratch_shapes=[
                pltpu.VMEM((spaces // 2, 16, 128), F32),
                pltpu.VMEM((8, spaces), jnp.int32),
                pltpu.SMEM((8, spaces), jnp.int32),
                pltpu.VMEM((group, rows, 128), F32),
                pltpu.VMEM((group, rows, 128), F32),
                pltpu.VMEM((na, 16, 384), F32),
                pltpu.VMEM((na, 16, 384), F32),
                dma, dma((group,)), dma((group,)), dma((na,)), dma((na,)),
            ],
            compiler_params=pltpu.CompilerParams(collective_id=0, has_side_effects=True),
            name="profiles",
        )(tile_halo, halo_owner, cell_bin.reshape(-1, TILE), cell_fields)

    in_specs = (P(("space", "rad")), P(None, ("space", "rad")), P(("space", "rad")), P())
    out_specs = (P("space", "rad"),) * 4
    return jax.shard_map(body, mesh=mesh, in_specs=in_specs, out_specs=out_specs, check_vma=False)
```

```python
import functools

import jax
import jax.numpy as jnp
from jax import lax
from jax.experimental import pallas as pl
from jax.experimental.pallas import tpu as pltpu
from jax.sharding import PartitionSpec as P

MESH = pl.DeviceIdType.MESH
F32 = jnp.float32
BF16 = jnp.bfloat16
TILE = 128
BINS = 256
QUARTER = 64
HALO_DEV = 32
log_inner = -2.302585092994046


def split3(v):
    high = v.astype(BF16)
    rest = v - high.astype(F32)
    mid = rest.astype(BF16)
    low = (rest - mid.astype(F32)).astype(BF16)
    return high, mid, low


def iota(shape, dim):
    return lax.broadcasted_iota(jnp.int32, shape, dim)


def nt(a, b):
    return lax.dot_general(a, b, (((1,), (1,)), ((), ())), preferred_element_type=F32)


def bin_piece(k, bin_ref, fld_ref):
    label = jnp.concatenate([bin_ref[pl.ds(2 * k, 1), :], bin_ref[pl.ds(2 * k + 1, 1), :]], axis=1)
    low = label & (QUARTER - 1)
    high = lax.shift_right_logical(label, 6)
    v = fld_ref[:, pl.ds(pl.multiple_of(2 * TILE * k, 2 * TILE), 2 * TILE)]
    pad = jnp.zeros((1, 2 * TILE), F32)
    v8 = jnp.concatenate([v, pad, v, pad], axis=0)
    row = iota((8, 2 * TILE), 0)
    parts = [[], [], []]
    bases = []
    for t in range(2):
        quarter = 2 * t + lax.shift_right_logical(row, 2)
        own = jnp.where(high == quarter, v8, 0.0)
        for s, part in enumerate(split3(own)):
            parts[s].append(part)
        bases.append(jnp.sum(jnp.where(high < quarter, v8, 0.0), axis=1, keepdims=True))
    lhs = jnp.concatenate(parts[0] + parts[1] + parts[2], axis=0)
    below = jnp.where(low <= iota((QUARTER, 2 * TILE), 0), 1.0, 0.0).astype(BF16)
    below = jnp.concatenate([below, below], axis=0)
    out = nt(lhs, below)
    out = out[0:16] + out[16:32] + out[32:48]
    return out + jnp.concatenate(bases, axis=0)


def kernel(na, nj, ny, halo_hbm, owner_hbm, bin_hbm, fld_hbm, got, halo_ref, owner_ref, bin_ref, fld_ref,
           pieces, code_v, code_s, send, recv, dense, in_sem, code_sem, send1, recv1, send2, recv2, own_sem):
    owners = na * nj
    count = owners // 2
    pairs = na // 2
    group = nj * ny
    rows = 3 * pairs + 1
    space = lax.axis_index("space")
    y = lax.axis_index("rad")
    a = space // nj
    j = space % nj
    me = j * ny + y

    chunks = min(4, count)
    size = count // chunks
    fetches = [pltpu.make_async_copy(halo_hbm, halo_ref, in_sem.at[0]),
               pltpu.make_async_copy(owner_hbm, owner_ref, in_sem.at[1])]
    for c in range(chunks):
        fetches.append(pltpu.make_async_copy(
            bin_hbm.at[2 * size * c:2 * size * (c + 1)], bin_ref.at[2 * size * c:2 * size * (c + 1)], in_sem.at[2 + 2 * c]))
        cells = slice(2 * TILE * size * c, 2 * TILE * size * (c + 1))
        fetches.append(pltpu.make_async_copy(fld_hbm.at[:, cells], fld_ref.at[:, cells], in_sem.at[3 + 2 * c]))
    for fetch in fetches:
        fetch.start()

    barrier = pltpu.get_barrier_semaphore()
    for i in range(1, na):
        pl.semaphore_signal(barrier, inc=1, device_id=(lax.rem(a + i, na) * nj + j, y), device_id_type=MESH)
    for dj in range(nj):
        for dy in range(ny):
            @pl.when(jnp.logical_or(dj != j, dy != y))
            def _():
                pl.semaphore_signal(barrier, inc=1, device_id=(a * nj + dj, dy), device_id_type=MESH)

    lane = iota((8, owners), 1)

    def note(k, codes):
        halo = halo_ref[2 * k]
        code = 1 + HALO_DEV * k + (halo & (HALO_DEV - 1))
        return jnp.where(lane == owner_ref[halo], code, codes)

    def piece_and_notes(k, codes):
        pieces[k] = bin_piece(k, bin_ref, fld_ref)
        return note(2 * k + 1, note(2 * k, codes))

    def one_piece(k, carry):
        pieces[k] = bin_piece(k, bin_ref, fld_ref)
        return carry

    noting = pltpu.make_async_copy(code_v, code_s, code_sem)
    fetches[0].wait()
    fetches[1].wait()
    codes = jnp.zeros((8, owners), jnp.int32)
    for c in range(chunks):
        fetches[2 + 2 * c].wait()
        fetches[3 + 2 * c].wait()
        if 2 * c < chunks:
            codes = lax.fori_loop(size * c, size * (c + 1), piece_and_notes, codes, unroll=size)
            if 2 * (c + 1) == chunks:
                code_v[...] = codes
                noting.start()
        else:
            lax.fori_loop(size * c, size * (c + 1), one_piece, 0, unroll=size)
    noting.wait()
    pl.semaphore_wait(barrier, group - 1 + na - 1)

    lane128 = iota((1, 128), 1)
    left = iota((16, 128), 1) < QUARTER
    tag = 128 // na

    def outbound(dj, dy):
        t = dj * ny + dy
        return pltpu.make_async_remote_copy(
            src_ref=send.at[t], dst_ref=recv.at[me], send_sem=send1.at[t], recv_sem=recv1.at[me],
            device_id=(a * nj + dj, dy), device_id_type=MESH)

    def assemble(i, carry):
        dj = lax.rem(j + 1 + i, nj)
        labels = jnp.zeros((1, 128), F32)
        for p in range(pairs):
            codes = [code_s[0, 2 * p * nj + dj], code_s[0, (2 * p + 1) * nj + dj]]
            held = [pieces[lax.shift_right_logical(jnp.maximum(c - 1, 0), 5)] for c in codes]
            there = [jnp.where(c > 0, 1, 0) for c in codes]
            both = jnp.where(left, held[0], held[1])
            both = jnp.where(jnp.where(left, there[0], there[1]) > 0, both, 0.0)
            for par in range(2):
                rank = jnp.where(codes[par] > 0, (codes[par] - 1) & (HALO_DEV - 1), -1).astype(F32)
                labels = jnp.where(lane128 // tag == 2 * p + par, rank, labels)
            for q in range(ny):
                send[dj * ny + q, 3 * p:3 * p + 3, :] = both[4 * q:4 * q + 3]
        for q in range(ny):
            send[dj * ny + q, rows - 1:rows, :] = labels
        for dy in range(ny):
            @pl.when(jnp.logical_or(dj != j, dy != y))
            def _():
                outbound(dj, dy).start()
        return carry

    lax.fori_loop(0, nj, assemble, 0)
    recv[me] = send[me]

    def inbound(t):
        return pltpu.make_async_remote_copy(
            src_ref=send.at[t], dst_ref=recv.at[t], send_sem=send1.at[t], recv_sem=recv1.at[t],
            device_id=(a * nj + t // ny, lax.rem(t, ny)), device_id_type=MESH)

    def arrive(i, carry):
        inbound(lax.rem(me + group - i, group)).wait_recv()
        return carry

    lax.fori_loop(1, group, arrive, 0)

    labels = recv[:, rows - 1, :].astype(BF16)
    labels = jnp.concatenate([labels] * 3, axis=0)
    spread = jnp.where(iota((na * HALO_DEV, 128), 1) == tag * (iota((na * HALO_DEV, 128), 0) // HALO_DEV), 1.0, 0.0).astype(BF16)
    spread = nt(spread, labels)
    wanted = (iota(spread.shape, 0) & (HALO_DEV - 1)).astype(F32)
    chosen = jnp.where(spread == wanted, 1.0, 0.0).astype(BF16)

    def onward(d):
        return pltpu.make_async_remote_copy(
            src_ref=dense.at[d], dst_ref=got.at[a], send_sem=send2.at[d], recv_sem=recv2.at[a],
            device_id=(d * nj + j, y), device_id_type=MESH)

    for p in range(pairs):
        columns = [jnp.concatenate(split3(recv[:, 3 * p + f, :]), axis=0) for f in range(3)]
        total = jnp.dot(chosen[2 * HALO_DEV * p:2 * HALO_DEV * (p + 1)], jnp.concatenate(columns, axis=1),
                        preferred_element_type=F32)
        for par in range(2):
            d = 2 * p + par
            for f in range(3):
                top = total[32 * par:32 * par + 16, 128 * f:128 * f + 128]
                bottom = total[32 * par + 16:32 * par + 32, 128 * f:128 * f + 128]
                if par == 0:
                    merged = jnp.where(left, top, pltpu.roll(bottom, QUARTER, 1))
                else:
                    merged = jnp.where(left, pltpu.roll(top, QUARTER, 1), bottom)
                dense[d, :, 128 * f:128 * f + 128] = merged

            @pl.when(d != a)
            def _():
                onward(d).start()

    keep = pltpu.make_async_copy(dense.at[a], got.at[a], own_sem)
    keep.start()
    for i in range(1, na):
        t = lax.rem(a + i, na)
        pltpu.make_async_remote_copy(
            src_ref=dense.at[t], dst_ref=got.at[t], send_sem=send2.at[t], recv_sem=recv2.at[t],
            device_id=(t * nj + j, y), device_id_type=MESH).wait_recv()
    keep.wait()

    def sent(i, carry):
        inbound(lax.rem(me + i, group)).wait_send()
        return carry

    lax.fori_loop(1, group, sent, 0)
    for i in range(1, na):
        onward(lax.rem(a + i, na)).wait_send()


def finish(na, got_ref, mass_ref, vol_ref, ent_ref, vel_ref):
    total = got_ref[0]
    for t in range(1, na):
        total = total + got_ref[t]
    bins = (lax.axis_index("rad") * QUARTER + 1 + iota((16, QUARTER), 1)).astype(F32)
    radius = jnp.exp(log_inner + bins * (-log_inner / BINS))
    for f, ref in enumerate((mass_ref, vol_ref, ent_ref)):
        block = total[:, 128 * f:128 * f + 128]
        for half, part in enumerate((block, pltpu.roll(block, QUARTER, 1))):
            part = part[:, :QUARTER]
            ref[16 * half:16 * half + 16, :] = part
            if f == 0:
                vel_ref[16 * half:16 * half + 16, :] = jnp.sqrt(part / radius)


def solution(mesh):
    spaces, ny = mesh.shape["space"], mesh.shape["rad"]
    na = 8 if spaces == 128 else 2
    nj = spaces // na
    group, rows = nj * ny, 3 * (na // 2) + 1

    def body(cell_bin, cell_fields, tile_halo, halo_owner):
        vmem = pl.BlockSpec(memory_space=pltpu.VMEM)
        anywhere = pl.BlockSpec(memory_space=pl.ANY)
        dma = pltpu.SemaphoreType.DMA
        out = jax.ShapeDtypeStruct((HALO_DEV, QUARTER), F32)
        got = pl.pallas_call(
            functools.partial(kernel, na, nj, ny),
            out_shape=jax.ShapeDtypeStruct((na, 16, 384), F32),
            in_specs=[anywhere] * 4,
            out_specs=anywhere,
            scratch_shapes=[
                pltpu.SMEM(tile_halo.shape, jnp.int32),
                pltpu.SMEM(halo_owner.shape, jnp.int32),
                pltpu.VMEM((tile_halo.shape[0], TILE), jnp.int32),
                pltpu.VMEM(cell_fields.shape, F32),
                pltpu.VMEM((spaces // 2, 16, 128), F32),
                pltpu.VMEM((8, spaces), jnp.int32),
                pltpu.SMEM((8, spaces), jnp.int32),
                pltpu.VMEM((group, rows, 128), F32),
                pltpu.VMEM((group, rows, 128), F32),
                pltpu.VMEM((na, 16, 384), F32),
                dma((10,)), dma, dma((group,)), dma((group,)), dma((na,)), dma((na,)), dma,
            ],
            compiler_params=pltpu.CompilerParams(collective_id=0, has_side_effects=True),
            name="profiles",
        )(tile_halo, halo_owner, cell_bin.reshape(-1, TILE), cell_fields)
        return pl.pallas_call(
            functools.partial(finish, na), out_shape=(out,) * 4, in_specs=[vmem], out_specs=(vmem,) * 4, name="finish",
        )(got)

    in_specs = (P(("space", "rad")), P(None, ("space", "rad")), P(("space", "rad")), P())
    out_specs = (P("space", "rad"),) * 4
    return jax.shard_map(body, mesh=mesh, in_specs=in_specs, out_specs=out_specs, check_vma=False)
```

```python
import functools

import jax
import jax.numpy as jnp
from jax import lax
from jax.experimental import pallas as pl
from jax.experimental.pallas import tpu as pltpu
from jax.sharding import PartitionSpec as P

MESH = pl.DeviceIdType.MESH
F32 = jnp.float32
BF16 = jnp.bfloat16
TILE = 128
BINS = 256
QUARTER = 64
HALO_DEV = 32
log_inner = -2.302585092994046


def split3(v):
    high = v.astype(BF16)
    rest = v - high.astype(F32)
    mid = rest.astype(BF16)
    low = (rest - mid.astype(F32)).astype(BF16)
    return high, mid, low


def iota(shape, dim):
    return lax.broadcasted_iota(jnp.int32, shape, dim)


def nt(a, b):
    return lax.dot_general(a, b, (((1,), (1,)), ((), ())), preferred_element_type=F32)


def bin_piece(k, bin_ref, fld_ref):
    label = jnp.concatenate([bin_ref[pl.ds(2 * k, 1), :], bin_ref[pl.ds(2 * k + 1, 1), :]], axis=1)
    low = label & (QUARTER - 1)
    high = lax.shift_right_logical(label, 6)
    v = fld_ref[:, pl.ds(pl.multiple_of(2 * TILE * k, 2 * TILE), 2 * TILE)]
    pad = jnp.zeros((1, 2 * TILE), F32)
    v8 = jnp.concatenate([v, pad, v, pad], axis=0)
    row = iota((8, 2 * TILE), 0)
    parts = [[], [], []]
    bases = []
    for t in range(2):
        quarter = 2 * t + lax.shift_right_logical(row, 2)
        own = jnp.where(high == quarter, v8, 0.0)
        for s, part in enumerate(split3(own)):
            parts[s].append(part)
        bases.append(jnp.sum(jnp.where(high < quarter, v8, 0.0), axis=1, keepdims=True))
    lhs = jnp.concatenate(parts[0] + parts[1] + parts[2], axis=0)
    below = jnp.where(low <= iota((QUARTER, 2 * TILE), 0), 1.0, 0.0).astype(BF16)
    below = jnp.concatenate([below, below], axis=0)
    out = nt(lhs, below)
    out = out[0:16] + out[16:32] + out[32:48]
    return out + jnp.concatenate(bases, axis=0)


def kernel(na, nj, ny, halo_hbm, owner_hbm, bin_hbm, fld_hbm, got, halo_ref, owner_ref, bin_ref, fld_ref,
           pieces, code_v, code_s, send, recv, dense, in_sem, code_sem, send1, recv1, send2, recv2):
    owners = na * nj
    count = owners // 2
    pairs = na // 2
    group = nj * ny
    space = lax.axis_index("space")
    y = lax.axis_index("rad")
    a = space // nj
    j = space % nj
    me = j * ny + y

    chunks = min(4, count)
    size = count // chunks
    fetches = [pltpu.make_async_copy(halo_hbm, halo_ref, in_sem.at[0]),
               pltpu.make_async_copy(owner_hbm, owner_ref, in_sem.at[1])]
    for c in range(chunks):
        fetches.append(pltpu.make_async_copy(
            bin_hbm.at[2 * size * c:2 * size * (c + 1)], bin_ref.at[2 * size * c:2 * size * (c + 1)], in_sem.at[2 + 2 * c]))
        cells = slice(2 * TILE * size * c, 2 * TILE * size * (c + 1))
        fetches.append(pltpu.make_async_copy(fld_hbm.at[:, cells], fld_ref.at[:, cells], in_sem.at[3 + 2 * c]))
    for fetch in fetches:
        fetch.start()

    barrier = pltpu.get_barrier_semaphore()
    for i in range(1, na):
        pl.semaphore_signal(barrier, inc=1, device_id=(lax.rem(a + i, na) * nj + j, y), device_id_type=MESH)
    for dj in range(nj):
        for dy in range(ny):
            @pl.when(jnp.logical_or(dj != j, dy != y))
            def _():
                pl.semaphore_signal(barrier, inc=1, device_id=(a * nj + dj, dy), device_id_type=MESH)

    lane = iota((8, owners), 1)

    def note(k, codes):
        halo = halo_ref[2 * k]
        code = 1 + HALO_DEV * k + (halo & (HALO_DEV - 1))
        return jnp.where(lane == owner_ref[halo], code, codes)

    def piece_and_notes(k, codes):
        pieces[k] = bin_piece(k, bin_ref, fld_ref)
        return note(2 * k + 1, note(2 * k, codes))

    def one_piece(k, carry):
        pieces[k] = bin_piece(k, bin_ref, fld_ref)
        return carry

    noting = pltpu.make_async_copy(code_v, code_s, code_sem)
    fetches[0].wait()
    fetches[1].wait()
    codes = jnp.zeros((8, owners), jnp.int32)
    for c in range(chunks):
        fetches[2 + 2 * c].wait()
        fetches[3 + 2 * c].wait()
        if 2 * c < chunks:
            codes = lax.fori_loop(size * c, size * (c + 1), piece_and_notes, codes, unroll=size)
            if 2 * (c + 1) == chunks:
                code_v[...] = codes
                noting.start()
        else:
            lax.fori_loop(size * c, size * (c + 1), one_piece, 0, unroll=size)
    noting.wait()
    pl.semaphore_wait(barrier, group - 1 + na - 1)

    left = iota((16, 128), 1) < QUARTER
    tagged = (iota((16, 128), 0) & 3) == 3
    first = (iota((16, 128), 1) & HALO_DEV) == 0

    def outbound(c, dj, dy):
        t = dj * ny + dy
        return pltpu.make_async_remote_copy(
            src_ref=send.at[c, t], dst_ref=recv.at[c, me], send_sem=send1.at[c], recv_sem=recv1.at[c],
            device_id=(a * nj + dj, dy), device_id_type=MESH)

    def everyone(c):
        return pltpu.make_async_remote_copy(
            src_ref=send.at[c, pl.ds(0, group - 1)], dst_ref=recv.at[c, pl.ds(0, group - 1)],
            send_sem=send1.at[c], recv_sem=recv1.at[c], device_id=(space, y), device_id_type=MESH)

    def onward(i):
        return pltpu.make_async_remote_copy(
            src_ref=dense.at[i], dst_ref=got.at[i], send_sem=send2.at[i], recv_sem=recv2.at[i],
            device_id=(lax.rem(a + i, na) * nj + j, y), device_id_type=MESH)

    order = [(na // 2 + p, na // 2 - 1 - p) for p in range(pairs)]

    for c, ahead in enumerate(order):
        bases = [lax.rem(a + i, na) * nj for i in ahead]

        def assemble(dj, carry):
            codes = [code_s[0, base + dj] for base in bases]
            held = [pieces[lax.shift_right_logical(jnp.maximum(code - 1, 0), 5)] for code in codes]
            there = [jnp.where(code > 0, 1, 0) for code in codes]
            ranks = [jnp.where(code > 0, (code - 1) & (HALO_DEV - 1), -1).astype(F32) for code in codes]
            both = jnp.where(left, held[0], held[1])
            both = jnp.where(jnp.where(left, there[0], there[1]) > 0, both, 0.0)
            both = jnp.where(tagged, jnp.where(first, ranks[0], ranks[1]), both)
            for q in range(ny):
                send[c, dj * ny + q] = both[4 * q:4 * q + 4]
            for dy in range(ny):
                @pl.when(jnp.logical_or(dj != j, dy != y))
                def _():
                    outbound(c, dj, dy).start()
            return carry

        lax.fori_loop(0, nj, assemble, 0, unroll=2)
        recv[c, me] = send[c, me]

    wanted = (iota((group, 128), 1) & (HALO_DEV - 1)).astype(F32)
    for c, ahead in enumerate(order):
        everyone(c).wait_recv()
        chosen = jnp.where(recv[c, :, 3, :] == wanted, 1.0, 0.0)
        chosen = chosen.T[:2 * HALO_DEV].astype(BF16)
        columns = [split3(recv[c, :, f, :]) for f in range(3)]
        total = sum(
            jnp.dot(chosen, jnp.concatenate([column[s] for column in columns], axis=1), preferred_element_type=F32)
            for s in range(3))
        for par, i in enumerate(ahead):
            for f in range(3):
                top = total[32 * par:32 * par + 16, 128 * f:128 * f + 128]
                bottom = total[32 * par + 16:32 * par + 32, 128 * f:128 * f + 128]
                if par == 0:
                    merged = jnp.where(left, top, pltpu.roll(bottom, QUARTER, 1))
                else:
                    merged = jnp.where(left, pltpu.roll(top, QUARTER, 1), bottom)
                (dense if i else got)[i, :, 128 * f:128 * f + 128] = merged
            if i:
                onward(i).start()

    for i in range(1, na):
        onward(i).wait_recv()
    for c in range(pairs):
        everyone(c).wait_send()
    for i in range(1, na):
        onward(i).wait_send()


def finish(na, got_ref, mass_ref, vol_ref, ent_ref, vel_ref):
    total = got_ref[0]
    for t in range(1, na):
        total = total + got_ref[t]
    bins = (lax.axis_index("rad") * QUARTER + 1 + iota((16, QUARTER), 1)).astype(F32)
    radius = jnp.exp(log_inner + bins * (-log_inner / BINS))
    for f, ref in enumerate((mass_ref, vol_ref, ent_ref)):
        block = total[:, 128 * f:128 * f + 128]
        for half, part in enumerate((block, pltpu.roll(block, QUARTER, 1))):
            part = part[:, :QUARTER]
            ref[16 * half:16 * half + 16, :] = part
            if f == 0:
                vel_ref[16 * half:16 * half + 16, :] = jnp.sqrt(part / radius)


def solution(mesh):
    spaces, ny = mesh.shape["space"], mesh.shape["rad"]
    na = 8 if spaces == 128 else 2
    nj = spaces // na
    group, pairs = nj * ny, na // 2

    def body(cell_bin, cell_fields, tile_halo, halo_owner):
        vmem = pl.BlockSpec(memory_space=pltpu.VMEM)
        anywhere = pl.BlockSpec(memory_space=pl.ANY)
        dma = pltpu.SemaphoreType.DMA
        out = jax.ShapeDtypeStruct((HALO_DEV, QUARTER), F32)
        got = pl.pallas_call(
            functools.partial(kernel, na, nj, ny),
            out_shape=pltpu.VMEM((na, 16, 384), F32),
            in_specs=[anywhere] * 4,
            out_specs=vmem,
            scratch_shapes=[
                pltpu.SMEM(tile_halo.shape, jnp.int32),
                pltpu.SMEM(halo_owner.shape, jnp.int32),
                pltpu.VMEM((tile_halo.shape[0], TILE), jnp.int32),
                pltpu.VMEM(cell_fields.shape, F32),
                pltpu.VMEM((spaces // 2, 16, 128), F32),
                pltpu.VMEM((8, spaces), jnp.int32),
                pltpu.SMEM((8, spaces), jnp.int32),
                pltpu.VMEM((pairs, group, 4, 128), F32),
                pltpu.VMEM((pairs, group, 4, 128), F32),
                pltpu.VMEM((na, 16, 384), F32),
                dma((10,)), dma, dma((pairs,)), dma((pairs,)), dma((na,)), dma((na,)),
            ],
            compiler_params=pltpu.CompilerParams(collective_id=0, has_side_effects=True),
            name="profiles",
        )(tile_halo, halo_owner, cell_bin.reshape(-1, TILE), cell_fields)
        return pl.pallas_call(
            functools.partial(finish, na), out_shape=(out,) * 4, in_specs=[vmem], out_specs=(vmem,) * 4, name="finish",
        )(pltpu.with_memory_space_constraint(got, pltpu.VMEM))

    in_specs = (P(("space", "rad")), P(None, ("space", "rad")), P(("space", "rad")), P())
    out_specs = (P("space", "rad"),) * 4
    return jax.shard_map(body, mesh=mesh, in_specs=in_specs, out_specs=out_specs, check_vma=False)
```

```python
import functools

import jax
import jax.numpy as jnp
from jax import lax
from jax.experimental import pallas as pl
from jax.experimental.pallas import tpu as pltpu
from jax.sharding import PartitionSpec as P

MESH = pl.DeviceIdType.MESH
F32 = jnp.float32
BF16 = jnp.bfloat16
TILE = 128
BINS = 256
QUARTER = 64
HALO_DEV = 32
log_inner = -2.302585092994046


def split3(v):
    high = v.astype(BF16)
    rest = v - high.astype(F32)
    mid = rest.astype(BF16)
    low = (rest - mid.astype(F32)).astype(BF16)
    return high, mid, low


def iota(shape, dim):
    return lax.broadcasted_iota(jnp.int32, shape, dim)


def nt(a, b):
    return lax.dot_general(a, b, (((1,), (1,)), ((), ())), preferred_element_type=F32)


def bin_piece(k, bin_ref, fld_ref):
    label = jnp.concatenate([bin_ref[pl.ds(2 * k, 1), :], bin_ref[pl.ds(2 * k + 1, 1), :]], axis=1)
    low = label & (QUARTER - 1)
    high = lax.shift_right_logical(label, 6)
    v = fld_ref[:, pl.ds(pl.multiple_of(2 * TILE * k, 2 * TILE), 2 * TILE)]
    pad = jnp.zeros((1, 2 * TILE), F32)
    v8 = jnp.concatenate([v, pad, v, pad], axis=0)
    row = iota((8, 2 * TILE), 0)
    parts = [[], [], []]
    bases = []
    for t in range(2):
        quarter = 2 * t + lax.shift_right_logical(row, 2)
        own = jnp.where(high == quarter, v8, 0.0)
        for s, part in enumerate(split3(own)):
            parts[s].append(part)
        bases.append(jnp.sum(jnp.where(high < quarter, v8, 0.0), axis=1, keepdims=True))
    lhs = jnp.concatenate(parts[0] + parts[1] + parts[2], axis=0)
    below = jnp.where(low <= iota((QUARTER, 2 * TILE), 0), 1.0, 0.0).astype(BF16)
    below = jnp.concatenate([below, below], axis=0)
    out = nt(lhs, below)
    out = out[0:16] + out[16:32] + out[32:48]
    return out + jnp.concatenate(bases, axis=0)


def kernel(na, nj, ny, halo_hbm, owner_hbm, bin_hbm, fld_hbm, got, halo_ref, owner_ref, bin_ref, fld_ref,
           pieces, code_v, code_s, send, recv, dense, in_sem, code_sem, send1, recv1, send2, recv2, ready1, ready2):
    owners = na * nj
    count = owners // 2
    pairs = na // 2
    group = nj * ny
    space = lax.axis_index("space")
    y = lax.axis_index("rad")
    a = space // nj
    j = space % nj
    me = j * ny + y

    chunks = min(4, count)
    size = count // chunks
    fetches = [pltpu.make_async_copy(halo_hbm, halo_ref, in_sem.at[0]),
               pltpu.make_async_copy(owner_hbm, owner_ref, in_sem.at[1])]
    for c in range(chunks):
        fetches.append(pltpu.make_async_copy(
            bin_hbm.at[2 * size * c:2 * size * (c + 1)], bin_ref.at[2 * size * c:2 * size * (c + 1)], in_sem.at[2 + 2 * c]))
        cells = slice(2 * TILE * size * c, 2 * TILE * size * (c + 1))
        fetches.append(pltpu.make_async_copy(fld_hbm.at[:, cells], fld_ref.at[:, cells], in_sem.at[3 + 2 * c]))
    for fetch in fetches:
        fetch.start()

    barrier = pltpu.get_barrier_semaphore()
    core = lax.rem(space, 2)
    sibling = space + 1 - 2 * core
    for dj in range(0, nj, 2):
        for dy in range(ny):
            @pl.when(jnp.logical_or(dj != j, dy != y))
            def _():
                pl.semaphore_signal(barrier, inc=1, device_id=(a * nj + dj, dy), device_id_type=MESH)
    for i in range(1, na):
        pl.semaphore_signal(
            barrier, inc=1, device_id=(lax.rem(a + i, na) * nj + j + 1 - core, y), device_id_type=MESH)

    lane = iota((8, owners), 1)

    def note(k, codes):
        halo = halo_ref[2 * k]
        code = 1 + HALO_DEV * k + (halo & (HALO_DEV - 1))
        return jnp.where(lane == owner_ref[halo], code, codes)

    def piece_and_notes(k, codes):
        pieces[k] = bin_piece(k, bin_ref, fld_ref)
        return note(2 * k + 1, note(2 * k, codes))

    def one_piece(k, carry):
        pieces[k] = bin_piece(k, bin_ref, fld_ref)
        return carry

    noting = pltpu.make_async_copy(code_v, code_s, code_sem)
    fetches[0].wait()
    fetches[1].wait()
    codes = jnp.zeros((8, owners), jnp.int32)
    for c in range(chunks):
        fetches[2 + 2 * c].wait()
        fetches[3 + 2 * c].wait()
        if 2 * c < chunks:
            codes = lax.fori_loop(size * c, size * (c + 1), piece_and_notes, codes, unroll=size)
            if 2 * (c + 1) == chunks:
                code_v[...] = codes
                noting.start()
        else:
            lax.fori_loop(size * c, size * (c + 1), one_piece, 0, unroll=size)
    noting.wait()

    @pl.when(core == 0)
    def _():
        pl.semaphore_wait(barrier, group - 1)
        pl.semaphore_signal(ready1, inc=1, device_id=(sibling, y), device_id_type=MESH)

    @pl.when(core == 1)
    def _():
        pl.semaphore_wait(ready1, 1)

    left = iota((16, 128), 1) < QUARTER
    tagged = (iota((16, 128), 0) & 3) == 3
    first = (iota((16, 128), 1) & HALO_DEV) == 0

    def outbound(c, dj, dy):
        t = dj * ny + dy
        return pltpu.make_async_remote_copy(
            src_ref=send.at[c, t], dst_ref=recv.at[c, me], send_sem=send1.at[c], recv_sem=recv1.at[c],
            device_id=(a * nj + dj, dy), device_id_type=MESH)

    def everyone(c):
        return pltpu.make_async_remote_copy(
            src_ref=send.at[c, pl.ds(0, group - 1)], dst_ref=recv.at[c, pl.ds(0, group - 1)],
            send_sem=send1.at[c], recv_sem=recv1.at[c], device_id=(space, y), device_id_type=MESH)

    def onward(i):
        return pltpu.make_async_remote_copy(
            src_ref=dense.at[i], dst_ref=got.at[i], send_sem=send2.at[i], recv_sem=recv2.at[i],
            device_id=(lax.rem(a + i, na) * nj + j, y), device_id_type=MESH)

    order = [(na // 2 + p, na // 2 - 1 - p) for p in range(pairs)]

    for c, ahead in enumerate(order):
        bases = [lax.rem(a + i, na) * nj for i in ahead]

        def assemble(dj, carry):
            codes = [code_s[0, base + dj] for base in bases]
            held = [pieces[lax.shift_right_logical(jnp.maximum(code - 1, 0), 5)] for code in codes]
            there = [jnp.where(code > 0, 1, 0) for code in codes]
            ranks = [jnp.where(code > 0, (code - 1) & (HALO_DEV - 1), -1).astype(F32) for code in codes]
            both = jnp.where(left, held[0], held[1])
            both = jnp.where(jnp.where(left, there[0], there[1]) > 0, both, 0.0)
            both = jnp.where(tagged, jnp.where(first, ranks[0], ranks[1]), both)
            for q in range(ny):
                send[c, dj * ny + q] = both[4 * q:4 * q + 4]
            for dy in range(ny):
                @pl.when(jnp.logical_or(dj != j, dy != y))
                def _():
                    outbound(c, dj, dy).start()
            return carry

        lax.fori_loop(0, nj, assemble, 0, unroll=2)
        recv[c, me] = send[c, me]

    wanted = (iota((group, 128), 1) & (HALO_DEV - 1)).astype(F32)
    for c, ahead in enumerate(order):
        everyone(c).wait_recv()
        chosen = jnp.where(recv[c, :, 3, :] == wanted, 1.0, 0.0)
        chosen = chosen.T[:2 * HALO_DEV].astype(BF16)
        columns = [split3(recv[c, :, f, :]) for f in range(3)]
        total = sum(
            jnp.dot(chosen, jnp.concatenate([column[s] for column in columns], axis=1), preferred_element_type=F32)
            for s in range(3))
        for par, i in enumerate(ahead):
            for f in range(3):
                top = total[32 * par:32 * par + 16, 128 * f:128 * f + 128]
                bottom = total[32 * par + 16:32 * par + 32, 128 * f:128 * f + 128]
                if par == 0:
                    merged = jnp.where(left, top, pltpu.roll(bottom, QUARTER, 1))
                else:
                    merged = jnp.where(left, pltpu.roll(top, QUARTER, 1), bottom)
                (dense if i else got)[i, :, 128 * f:128 * f + 128] = merged
            if i == order[0][0]:
                @pl.when(core == 1)
                def _():
                    pl.semaphore_wait(barrier, 2 * (na - 1))
                    pl.semaphore_signal(ready2, inc=1, device_id=(sibling, y), device_id_type=MESH)

                @pl.when(core == 0)
                def _():
                    pl.semaphore_wait(ready2, 1)
            if i:
                onward(i).start()

    for i in range(1, na):
        onward(i).wait_recv()
    for c in range(pairs):
        everyone(c).wait_send()
    for i in range(1, na):
        onward(i).wait_send()


def finish(na, got_ref, mass_ref, vol_ref, ent_ref, vel_ref):
    total = got_ref[0]
    for t in range(1, na):
        total = total + got_ref[t]
    bins = (lax.axis_index("rad") * QUARTER + 1 + iota((16, QUARTER), 1)).astype(F32)
    radius = jnp.exp(log_inner + bins * (-log_inner / BINS))
    for f, ref in enumerate((mass_ref, vol_ref, ent_ref)):
        block = total[:, 128 * f:128 * f + 128]
        for half, part in enumerate((block, pltpu.roll(block, QUARTER, 1))):
            part = part[:, :QUARTER]
            ref[16 * half:16 * half + 16, :] = part
            if f == 0:
                vel_ref[16 * half:16 * half + 16, :] = jnp.sqrt(part / radius)


def solution(mesh):
    spaces, ny = mesh.shape["space"], mesh.shape["rad"]
    na = 8 if spaces == 128 else 2
    nj = spaces // na
    group, pairs = nj * ny, na // 2

    def body(cell_bin, cell_fields, tile_halo, halo_owner):
        vmem = pl.BlockSpec(memory_space=pltpu.VMEM)
        anywhere = pl.BlockSpec(memory_space=pl.ANY)
        dma = pltpu.SemaphoreType.DMA
        out = jax.ShapeDtypeStruct((HALO_DEV, QUARTER), F32)
        got = pl.pallas_call(
            functools.partial(kernel, na, nj, ny),
            out_shape=pltpu.VMEM((na, 16, 384), F32),
            in_specs=[anywhere] * 4,
            out_specs=vmem,
            scratch_shapes=[
                pltpu.SMEM(tile_halo.shape, jnp.int32),
                pltpu.SMEM(halo_owner.shape, jnp.int32),
                pltpu.VMEM((tile_halo.shape[0], TILE), jnp.int32),
                pltpu.VMEM(cell_fields.shape, F32),
                pltpu.VMEM((spaces // 2, 16, 128), F32),
                pltpu.VMEM((8, spaces), jnp.int32),
                pltpu.SMEM((8, spaces), jnp.int32),
                pltpu.VMEM((pairs, group, 4, 128), F32),
                pltpu.VMEM((pairs, group, 4, 128), F32),
                pltpu.VMEM((na, 16, 384), F32),
                dma((10,)), dma, dma((pairs,)), dma((pairs,)), dma((na,)), dma((na,)),
                pltpu.SemaphoreType.REGULAR, pltpu.SemaphoreType.REGULAR,
            ],
            compiler_params=pltpu.CompilerParams(collective_id=0, has_side_effects=True),
            name="profiles",
        )(tile_halo, halo_owner, cell_bin.reshape(-1, TILE), cell_fields)
        return pl.pallas_call(
            functools.partial(finish, na), out_shape=(out,) * 4, in_specs=[vmem], out_specs=(vmem,) * 4, name="finish",
        )(pltpu.with_memory_space_constraint(got, pltpu.VMEM))

    in_specs = (P(("space", "rad")), P(None, ("space", "rad")), P(("space", "rad")), P())
    out_specs = (P("space", "rad"),) * 4
    return jax.shard_map(body, mesh=mesh, in_specs=in_specs, out_specs=out_specs, check_vma=False)
```

```python
import functools

import jax
import jax.numpy as jnp
from jax import lax
from jax.experimental import pallas as pl
from jax.experimental.pallas import tpu as pltpu
from jax.sharding import PartitionSpec as P

MESH = pl.DeviceIdType.MESH
F32 = jnp.float32
BF16 = jnp.bfloat16
TILE = 128
BINS = 256
QUARTER = 64
HALO_DEV = 32
log_inner = -2.302585092994046


def split3(v):
    high = v.astype(BF16)
    rest = v - high.astype(F32)
    mid = rest.astype(BF16)
    low = (rest - mid.astype(F32)).astype(BF16)
    return high, mid, low


def iota(shape, dim):
    return lax.broadcasted_iota(jnp.int32, shape, dim)


def nt(a, b):
    return lax.dot_general(a, b, (((1,), (1,)), ((), ())), preferred_element_type=F32)


def bin_piece(k, bin_ref, fld_ref):
    label = jnp.concatenate([bin_ref[pl.ds(2 * k, 1), :], bin_ref[pl.ds(2 * k + 1, 1), :]], axis=1)
    low = label & (QUARTER - 1)
    high = lax.shift_right_logical(label, 6)
    v = fld_ref[:, pl.ds(pl.multiple_of(2 * TILE * k, 2 * TILE), 2 * TILE)]
    pad = jnp.zeros((1, 2 * TILE), F32)
    v8 = jnp.concatenate([v, pad, v, pad], axis=0)
    row = iota((8, 2 * TILE), 0)
    parts = [[], [], []]
    bases = []
    for t in range(2):
        quarter = 2 * t + lax.shift_right_logical(row, 2)
        own = jnp.where(high == quarter, v8, 0.0)
        for s, part in enumerate(split3(own)):
            parts[s].append(part)
        bases.append(jnp.sum(jnp.where(high < quarter, v8, 0.0), axis=1, keepdims=True))
    lhs = jnp.concatenate(parts[0] + parts[1] + parts[2], axis=0)
    below = jnp.where(low <= iota((QUARTER, 2 * TILE), 0), 1.0, 0.0).astype(BF16)
    below = jnp.concatenate([below, below], axis=0)
    out = nt(lhs, below)
    out = out[0:16] + out[16:32] + out[32:48]
    return out + jnp.concatenate(bases, axis=0)


def kernel(na, nj, ny, halo_hbm, owner_hbm, bin_hbm, fld_hbm, got, halo_ref, owner_ref, bin_ref, fld_ref,
           pieces, code_v, code_s, send, recv, dense, in_sem, code_sem, send1, recv1, send2, recv2, ready1, ready2):
    owners = na * nj
    count = owners // 2
    pairs = na // 2
    group = nj * ny
    space = lax.axis_index("space")
    y = lax.axis_index("rad")
    a = space // nj
    j = space % nj
    me = j * ny + y

    chunks = min(4, count)
    size = count // chunks
    fetches = [pltpu.make_async_copy(halo_hbm, halo_ref, in_sem.at[0]),
               pltpu.make_async_copy(owner_hbm, owner_ref, in_sem.at[1])]
    for c in range(chunks):
        fetches.append(pltpu.make_async_copy(
            bin_hbm.at[2 * size * c:2 * size * (c + 1)], bin_ref.at[2 * size * c:2 * size * (c + 1)], in_sem.at[2 + 2 * c]))
        cells = slice(2 * TILE * size * c, 2 * TILE * size * (c + 1))
        fetches.append(pltpu.make_async_copy(fld_hbm.at[:, cells], fld_ref.at[:, cells], in_sem.at[3 + 2 * c]))
    for fetch in fetches:
        fetch.start()

    def across(t, dj):
        d = lax.rem(t + na - a, na)
        half = na // 2
        return lax.rem(dj + (nj // 2) * (d // half) * (1 - (lax.rem(d, half) + half - 1) // half), nj)

    barrier = pltpu.get_barrier_semaphore()
    core = lax.rem(space, 2)
    sibling = space + 1 - 2 * core
    for dj in range(0, nj, 2):
        for dy in range(ny):
            @pl.when(jnp.logical_or(dj != j, dy != y))
            def _():
                pl.semaphore_signal(barrier, inc=1, device_id=(a * nj + dj, dy), device_id_type=MESH)
    for i in range(1, na):
        t = lax.rem(a + i, na)
        pl.semaphore_signal(barrier, inc=1, device_id=(t * nj + across(t, j) // 2 * 2 + 1, y), device_id_type=MESH)

    lane = iota((8, owners), 1)

    def note(k, codes):
        halo = halo_ref[2 * k]
        code = 1 + HALO_DEV * k + (halo & (HALO_DEV - 1))
        return jnp.where(lane == owner_ref[halo], code, codes)

    def piece_and_notes(k, codes):
        pieces[k] = bin_piece(k, bin_ref, fld_ref)
        return note(2 * k + 1, note(2 * k, codes))

    def one_piece(k, carry):
        pieces[k] = bin_piece(k, bin_ref, fld_ref)
        return carry

    noting = pltpu.make_async_copy(code_v, code_s, code_sem)
    fetches[0].wait()
    fetches[1].wait()
    codes = jnp.zeros((8, owners), jnp.int32)
    for c in range(chunks):
        fetches[2 + 2 * c].wait()
        fetches[3 + 2 * c].wait()
        if 2 * c < chunks:
            codes = lax.fori_loop(size * c, size * (c + 1), piece_and_notes, codes, unroll=size)
            if 2 * (c + 1) == chunks:
                code_v[...] = codes
                noting.start()
        else:
            lax.fori_loop(size * c, size * (c + 1), one_piece, 0, unroll=size)
    noting.wait()

    @pl.when(core == 0)
    def _():
        pl.semaphore_wait(barrier, group - 1)
        pl.semaphore_signal(ready1, inc=1, device_id=(sibling, y), device_id_type=MESH)

    @pl.when(core == 1)
    def _():
        pl.semaphore_wait(ready1, 1)

    left = iota((16, 128), 1) < QUARTER
    tagged = (iota((16, 128), 0) & 3) == 3
    first = (iota((16, 128), 1) & HALO_DEV) == 0

    def outbound(c, dj, dy):
        t = dj * ny + dy
        return pltpu.make_async_remote_copy(
            src_ref=send.at[c, t], dst_ref=recv.at[c, me], send_sem=send1.at[c], recv_sem=recv1.at[c],
            device_id=(a * nj + dj, dy), device_id_type=MESH)

    def everyone(c):
        return pltpu.make_async_remote_copy(
            src_ref=send.at[c, pl.ds(0, group - 1)], dst_ref=recv.at[c, pl.ds(0, group - 1)],
            send_sem=send1.at[c], recv_sem=recv1.at[c], device_id=(space, y), device_id_type=MESH)

    def onward(t, slot):
        return pltpu.make_async_remote_copy(
            src_ref=dense.at[t], dst_ref=got.at[slot], send_sem=send2.at[t], recv_sem=recv2.at[slot],
            device_id=(t * nj + across(t, j), y), device_id_type=MESH)

    order = [(2 * p, 2 * p + 1) for p in range(pairs)]
    plane = nj // 4 if nj == 16 else 1

    for c, targets in enumerate(order):

        def assemble(k, turn):
            if nj == 16:
                dj = lax.rem(j // 2 + turn, 4) * 2 + (k // 2) * 8 + lax.rem(k, 2)
            else:
                dj = lax.rem(j + turn, nj)
            codes = [code_s[0, t * nj + across(t, dj)] for t in targets]
            held = [pieces[lax.shift_right_logical(jnp.maximum(code - 1, 0), 5)] for code in codes]
            there = [jnp.where(code > 0, 1, 0) for code in codes]
            ranks = [jnp.where(code > 0, (code - 1) & (HALO_DEV - 1), -1).astype(F32) for code in codes]
            both = jnp.where(left, held[0], held[1])
            both = jnp.where(jnp.where(left, there[0], there[1]) > 0, both, 0.0)
            both = jnp.where(tagged, jnp.where(first, ranks[0], ranks[1]), both)
            for q in range(ny):
                send[c, dj * ny + q] = both[4 * q:4 * q + 4]
            for turn_y in (2, 1, 3, 0):
                dy = lax.rem(y + turn_y, ny)
                if turn_y:
                    outbound(c, dj, dy).start()
                else:
                    @pl.when(dj != j)
                    def _():
                        outbound(c, dj, dy).start()
            return turn

        for turn in (2, 1, 3, 0) if nj == 16 else range(nj):
            lax.fori_loop(0, plane, assemble, turn, unroll=2)
        recv[c, me] = send[c, me]

    wanted = (iota((group, 128), 1) & (HALO_DEV - 1)).astype(F32)
    for c, targets in enumerate(order):
        everyone(c).wait_recv()
        chosen = jnp.where(recv[c, :, 3, :] == wanted, 1.0, 0.0)
        chosen = chosen.T[:2 * HALO_DEV].astype(BF16)
        columns = [split3(recv[c, :, f, :]) for f in range(3)]
        total = sum(
            jnp.dot(chosen, jnp.concatenate([column[s] for column in columns], axis=1), preferred_element_type=F32)
            for s in range(3))
        for par, t in enumerate(targets):
            for f in range(3):
                top = total[32 * par:32 * par + 16, 128 * f:128 * f + 128]
                bottom = total[32 * par + 16:32 * par + 32, 128 * f:128 * f + 128]
                if par == 0:
                    merged = jnp.where(left, top, pltpu.roll(bottom, QUARTER, 1))
                else:
                    merged = jnp.where(left, pltpu.roll(top, QUARTER, 1), bottom)
                dense[t, :, 128 * f:128 * f + 128] = merged
            if t == 0:
                @pl.when(core == 1)
                def _():
                    pl.semaphore_wait(barrier, 2 * (na - 1))
                    pl.semaphore_signal(ready2, inc=1, device_id=(sibling, y), device_id_type=MESH)

                @pl.when(core == 0)
                def _():
                    pl.semaphore_wait(ready2, 1)

            @pl.when(t != a)
            def _():
                onward(t, a).start()

    got[a] = dense[a]
    for i in range(1, na):
        t = lax.rem(a + i, na)
        onward(t, t).wait_recv()
    for c in range(pairs):
        everyone(c).wait_send()
    for i in range(1, na):
        t = lax.rem(a + i, na)
        onward(t, t).wait_send()


def finish(na, got_ref, mass_ref, vol_ref, ent_ref, vel_ref):
    total = got_ref[0]
    for t in range(1, na):
        total = total + got_ref[t]
    bins = (lax.axis_index("rad") * QUARTER + 1 + iota((16, QUARTER), 1)).astype(F32)
    radius = jnp.exp(log_inner + bins * (-log_inner / BINS))
    for f, ref in enumerate((mass_ref, vol_ref, ent_ref)):
        block = total[:, 128 * f:128 * f + 128]
        for half, part in enumerate((block, pltpu.roll(block, QUARTER, 1))):
            part = part[:, :QUARTER]
            ref[16 * half:16 * half + 16, :] = part
            if f == 0:
                vel_ref[16 * half:16 * half + 16, :] = jnp.sqrt(part / radius)


def solution(mesh):
    spaces, ny = mesh.shape["space"], mesh.shape["rad"]
    na = 8 if spaces == 128 else 2
    nj = spaces // na
    group, pairs = nj * ny, na // 2

    def body(cell_bin, cell_fields, tile_halo, halo_owner):
        vmem = pl.BlockSpec(memory_space=pltpu.VMEM)
        anywhere = pl.BlockSpec(memory_space=pl.ANY)
        dma = pltpu.SemaphoreType.DMA
        out = jax.ShapeDtypeStruct((HALO_DEV, QUARTER), F32)
        got = pl.pallas_call(
            functools.partial(kernel, na, nj, ny),
            out_shape=pltpu.VMEM((na, 16, 384), F32),
            in_specs=[anywhere] * 4,
            out_specs=vmem,
            scratch_shapes=[
                pltpu.SMEM(tile_halo.shape, jnp.int32),
                pltpu.SMEM(halo_owner.shape, jnp.int32),
                pltpu.VMEM((tile_halo.shape[0], TILE), jnp.int32),
                pltpu.VMEM(cell_fields.shape, F32),
                pltpu.VMEM((spaces // 2, 16, 128), F32),
                pltpu.VMEM((8, spaces), jnp.int32),
                pltpu.SMEM((8, spaces), jnp.int32),
                pltpu.VMEM((pairs, group, 4, 128), F32),
                pltpu.VMEM((pairs, group, 4, 128), F32),
                pltpu.VMEM((na, 16, 384), F32),
                dma((10,)), dma, dma((pairs,)), dma((pairs,)), dma((na,)), dma((na,)),
                pltpu.SemaphoreType.REGULAR, pltpu.SemaphoreType.REGULAR,
            ],
            compiler_params=pltpu.CompilerParams(collective_id=0, has_side_effects=True),
            name="profiles",
        )(tile_halo, halo_owner, cell_bin.reshape(-1, TILE), cell_fields)
        return pl.pallas_call(
            functools.partial(finish, na), out_shape=(out,) * 4, in_specs=[vmem], out_specs=(vmem,) * 4, name="finish",
        )(pltpu.with_memory_space_constraint(got, pltpu.VMEM))

    in_specs = (P(("space", "rad")), P(None, ("space", "rad")), P(("space", "rad")), P())
    out_specs = (P("space", "rad"),) * 4
    return jax.shard_map(body, mesh=mesh, in_specs=in_specs, out_specs=out_specs, check_vma=False)
```

```python
import functools

import jax
import jax.numpy as jnp
from jax import lax
from jax.experimental import pallas as pl
from jax.experimental.pallas import tpu as pltpu
from jax.sharding import PartitionSpec as P

MESH = pl.DeviceIdType.MESH
F32 = jnp.float32
BF16 = jnp.bfloat16
TILE = 128
BINS = 256
QUARTER = 64
HALO_DEV = 32
log_inner = -2.302585092994046
AHEAD = 3


def halves(v):
    high = v.astype(BF16).astype(F32)
    return high, v - high


def iota(shape, dim):
    return lax.broadcasted_iota(jnp.int32, shape, dim)


def nt(a, b):
    return lax.dot_general(a, b, (((1,), (1,)), ((), ())), preferred_element_type=F32)


def bin_piece(k, bin_ref, fld_ref):
    label = jnp.concatenate([bin_ref[pl.ds(2 * k, 1), :], bin_ref[pl.ds(2 * k + 1, 1), :]], axis=1)
    low = label & (QUARTER - 1)
    high = lax.shift_right_logical(label, 6)
    v = fld_ref[:, pl.ds(pl.multiple_of(2 * TILE * k, 2 * TILE), 2 * TILE)]
    pad = jnp.zeros((1, 2 * TILE), F32)
    v8 = jnp.concatenate([v, pad, v, pad], axis=0)
    row = iota((8, 2 * TILE), 0)
    quarters = [2 * t + lax.shift_right_logical(row, 2) for t in range(2)]
    lhs = jnp.concatenate([jnp.where(high == q, part, 0.0) for part in halves(v8) for q in quarters], axis=0)
    bases = [jnp.sum(jnp.where(high < q, v8, 0.0), axis=1, keepdims=True) for q in quarters]
    below = jnp.where(low <= iota((QUARTER, 2 * TILE), 0), 1.0, 0.0).astype(BF16)
    below = jnp.concatenate([below, below], axis=0)
    out = nt(lhs.astype(BF16), below)
    return out[0:16] + out[16:32] + jnp.concatenate(bases, axis=0)


def kernel(na, nj, ny, halo_hbm, owner_hbm, bin_hbm, fld_hbm, sums, halo_ref, owner_ref, bin_ref, fld_ref,
           pieces, code_v, code_s, send_first, recv_first, send_rest, recv_rest, dense, got, in_sem, code_sem, send1, recv1, send2, recv2, ready1, ready2):
    owners = na * nj
    count = owners // 2
    pairs = na // 2
    group = nj * ny
    space = lax.axis_index("space")
    y = lax.axis_index("rad")
    a = space // nj
    j = space % nj
    me = j * ny + y

    chunks = min(2, count)
    size = count // chunks
    fetches = [pltpu.make_async_copy(halo_hbm, halo_ref, in_sem.at[0]),
               pltpu.make_async_copy(owner_hbm, owner_ref, in_sem.at[1])]
    for c in range(chunks):
        fetches.append(pltpu.make_async_copy(
            bin_hbm.at[2 * size * c:2 * size * (c + 1)], bin_ref.at[2 * size * c:2 * size * (c + 1)], in_sem.at[2 + 2 * c]))
        cells = slice(2 * TILE * size * c, 2 * TILE * size * (c + 1))
        fetches.append(pltpu.make_async_copy(fld_hbm.at[:, cells], fld_ref.at[:, cells], in_sem.at[3 + 2 * c]))
    for fetch in fetches:
        fetch.start()

    def across(t, dj):
        d = lax.rem(t + na - a, na)
        half = na // 2
        return lax.rem(dj + (nj // 2) * (d // half) * (1 - (lax.rem(d, half) + half - 1) // half), nj)

    barrier = pltpu.get_barrier_semaphore()
    core = lax.rem(space, 2)
    sibling = space + 1 - 2 * core
    for dj in range(0, nj, 2):
        for dy in range(ny):
            @pl.when(jnp.logical_or(dj != j, dy != y))
            def _():
                pl.semaphore_signal(barrier, inc=1, device_id=(a * nj + dj, dy), device_id_type=MESH)
    for i in range(1, na):
        t = lax.rem(a + i, na)
        pl.semaphore_signal(barrier, inc=1, device_id=(t * nj + across(t, j) // 2 * 2 + 1, y), device_id_type=MESH)

    lane = iota((8, owners), 1)

    def note(k, codes):
        halo = halo_ref[2 * k]
        code = HALO_DEV * k + (halo & (HALO_DEV - 1))
        return jnp.where(lane == owner_ref[halo], code, codes)

    def piece_and_notes(k, codes):
        pieces[k] = bin_piece(k, bin_ref, fld_ref)
        return note(2 * k + 1, note(2 * k, codes))

    def one_piece(k, carry):
        pieces[k] = bin_piece(k, bin_ref, fld_ref)
        return carry

    noting = pltpu.make_async_copy(code_v, code_s, code_sem)
    fetches[0].wait()
    fetches[1].wait()
    codes = jnp.full((8, owners), HALO_DEV * count, jnp.int32)
    pieces[count] = jnp.zeros((16, 128), F32)
    for c in range(chunks):
        fetches[2 + 2 * c].wait()
        fetches[3 + 2 * c].wait()
        if 2 * c < chunks:
            codes = lax.fori_loop(size * c, size * (c + 1), piece_and_notes, codes, unroll=size)
            if 2 * (c + 1) == chunks:
                code_v[...] = codes
                noting.start()
        else:
            lax.fori_loop(size * c, size * (c + 1), one_piece, 0, unroll=size)
    noting.wait()

    @pl.when(core == 0)
    def _():
        pl.semaphore_wait(barrier, group - 1)
        pl.semaphore_signal(ready1, inc=1, device_id=(sibling, y), device_id_type=MESH)

    @pl.when(core == 1)
    def _():
        pl.semaphore_wait(ready1, 1)

    left = iota((16, 128), 1) < QUARTER
    tagged = (iota((16, 128), 0) & 3) == 3
    block = lax.shift_right_logical(iota((8, 128), 1), 4)
    send = [send_first] + [send_rest.at[c] for c in range(pairs - 1)]
    recv = [recv_first] + [recv_rest.at[c] for c in range(pairs - 1)]

    def outbound(c, dj, dy):
        t = dj * ny + dy
        return pltpu.make_async_remote_copy(
            src_ref=send[c].at[t], dst_ref=recv[c].at[me], send_sem=send1.at[c], recv_sem=recv1.at[c],
            device_id=(a * nj + dj, dy), device_id_type=MESH)

    def everyone(c):
        return pltpu.make_async_remote_copy(
            src_ref=send[c].at[pl.ds(0, group - 1)], dst_ref=recv[c].at[pl.ds(0, group - 1)],
            send_sem=send1.at[c], recv_sem=recv1.at[c], device_id=(space, y), device_id_type=MESH)

    def onward(t, slot):
        return pltpu.make_async_remote_copy(
            src_ref=dense.at[t], dst_ref=got.at[slot], send_sem=send2.at[t], recv_sem=recv2.at[slot],
            device_id=(t * nj + across(t, j), y), device_id_type=MESH)

    order = [(2 * p, 2 * p + 1) for p in range(pairs)]

    def dispatch(c):
        for turn in (2, 1, 3, 0) if nj == 16 else range(nj):
            if nj == 16:
                dests = [lax.rem(j // 2 + turn, 4) * 2 + 8 * (k % 2) + k // 2 for k in range(4)]
            else:
                dests = [lax.rem(j + turn, nj)]
            for dj in dests:
                codes = [code_s[0, t * nj + across(t, dj)] for t in order[c]]
                held = [pieces[lax.shift_right_logical(code, 5)] for code in codes]
                both = jnp.where(left, held[0], held[1])
                if c == 0:
                    ranks = jnp.zeros((8, 128), jnp.int32)
                    for n, t in enumerate(sum(order, ())):
                        rank = code_s[0, t * nj + across(t, dj)] & (HALO_DEV - 1)
                        ranks = jnp.where(block == n, rank, ranks)
                    ranks = ranks.astype(F32)
                    both = jnp.where(tagged, jnp.concatenate([ranks, ranks], axis=0), both)
                for q in range(ny):
                    send[c][dj * ny + q] = both[4 * q:4 * q + (3 if c else 4)]
            for dj in dests:
                for turn_y in (2, 1, 3, 0):
                    dy = lax.rem(y + turn_y, ny)
                    if turn or turn_y:
                        outbound(c, dj, dy).start()
                    else:
                        @pl.when(dj != j)
                        def _():
                            outbound(c, dj, dy).start()
        recv[c][me] = send[c][me]

    for c in range(min(AHEAD, pairs)):
        dispatch(c)

    @pl.when(core == 1)
    def _():
        pl.semaphore_wait(barrier, 2 * (na - 1))
        pl.semaphore_signal(ready2, inc=1, device_id=(sibling, y), device_id_type=MESH)

    for c, targets in enumerate(order):
        everyone(c).wait_recv()
        if c == 0:
            labels = recv_first[:, 3, :]
            wanted = lax.rem(iota((group, 128), 1), 16)
            chosen = [jnp.where(labels == (wanted + 16 * half).astype(F32), 1.0, 0.0).T.astype(BF16) for half in range(2)]
        lhs = jnp.concatenate([rows[32 * c:32 * (c + 1)] for rows in chosen], axis=0)
        columns = [halves(recv[c][:, f, :]) for f in range(3)]
        total = sum(
            jnp.dot(lhs, jnp.concatenate([column[s] for column in columns], axis=1).astype(BF16), preferred_element_type=F32)
            for s in range(2))
        for par, t in enumerate(targets):
            for f in range(3):
                top = total[16 * par:16 * par + 16, 128 * f:128 * f + 128]
                bottom = total[16 * par + 32:16 * par + 48, 128 * f:128 * f + 128]
                if par == 0:
                    merged = jnp.where(left, top, pltpu.roll(bottom, QUARTER, 1))
                else:
                    merged = jnp.where(left, pltpu.roll(top, QUARTER, 1), bottom)
                dense[t, :, 128 * f:128 * f + 128] = merged
            if c == 0 and par == 0:
                @pl.when(core == 0)
                def _():
                    pl.semaphore_wait(ready2, 1)

            @pl.when(t != a)
            def _():
                onward(t, a).start()

        if c + AHEAD < pairs:
            dispatch(c + AHEAD)

    for c in range(pairs):
        everyone(c).wait_send()
    for i in range(1, na):
        t = lax.rem(a + i, na)
        onward(t, t).wait_send()
    total = dense[a]
    for i in range(1, na):
        t = lax.rem(a + i, na)
        onward(t, t).wait_recv()
        total = total + got[t]
    sums[...] = total


def finish(sums_ref, mass_ref, vol_ref, ent_ref, vel_ref):
    total = sums_ref[...]
    bins = (lax.axis_index("rad") * QUARTER + 1 + iota((16, QUARTER), 1)).astype(F32)
    radius = jnp.exp(log_inner + bins * (-log_inner / BINS))
    for f, ref in enumerate((mass_ref, vol_ref, ent_ref)):
        block = total[:, 128 * f:128 * f + 128]
        for half, part in enumerate((block, pltpu.roll(block, QUARTER, 1))):
            part = part[:, :QUARTER]
            ref[16 * half:16 * half + 16, :] = part
            if f == 0:
                vel_ref[16 * half:16 * half + 16, :] = jnp.sqrt(part / radius)


def solution(mesh):
    spaces, ny = mesh.shape["space"], mesh.shape["rad"]
    na = 8 if spaces == 128 else 2
    nj = spaces // na
    group, pairs = nj * ny, na // 2

    def body(cell_bin, cell_fields, tile_halo, halo_owner):
        vmem = pl.BlockSpec(memory_space=pltpu.VMEM)
        anywhere = pl.BlockSpec(memory_space=pl.ANY)
        dma = pltpu.SemaphoreType.DMA
        out = jax.ShapeDtypeStruct((HALO_DEV, QUARTER), F32)
        sums = pl.pallas_call(
            functools.partial(kernel, na, nj, ny),
            out_shape=pltpu.VMEM((16, 384), F32),
            in_specs=[anywhere] * 4,
            out_specs=vmem,
            scratch_shapes=[
                pltpu.SMEM(tile_halo.shape, jnp.int32),
                pltpu.SMEM(halo_owner.shape, jnp.int32),
                pltpu.VMEM((tile_halo.shape[0], TILE), jnp.int32),
                pltpu.VMEM(cell_fields.shape, F32),
                pltpu.VMEM((spaces // 2 + 1, 16, 128), F32),
                pltpu.VMEM((8, spaces), jnp.int32),
                pltpu.SMEM((8, spaces), jnp.int32),
                pltpu.VMEM((group, 4, 128), F32),
                pltpu.VMEM((group, 4, 128), F32),
                pltpu.VMEM((max(pairs - 1, 1), group, 3, 128), F32),
                pltpu.VMEM((max(pairs - 1, 1), group, 3, 128), F32),
                pltpu.VMEM((na, 16, 384), F32),
                pltpu.VMEM((na, 16, 384), F32),
                dma((10,)), dma, dma((pairs,)), dma((pairs,)), dma((na,)), dma((na,)),
                pltpu.SemaphoreType.REGULAR, pltpu.SemaphoreType.REGULAR,
            ],
            compiler_params=pltpu.CompilerParams(collective_id=0, has_side_effects=True),
            name="profiles",
        )(tile_halo, halo_owner, cell_bin.reshape(-1, TILE), cell_fields)
        return pl.pallas_call(
            finish, out_shape=(out,) * 4, in_specs=[vmem], out_specs=(vmem,) * 4, name="finish",
        )(pltpu.with_memory_space_constraint(sums, pltpu.VMEM))

    in_specs = (P(("space", "rad")), P(None, ("space", "rad")), P(("space", "rad")), P())
    out_specs = (P("space", "rad"),) * 4
    return jax.shard_map(body, mesh=mesh, in_specs=in_specs, out_specs=out_specs, check_vma=False)
```

```python
import functools

import jax
import jax.numpy as jnp
from jax import lax
from jax.experimental import pallas as pl
from jax.experimental.pallas import tpu as pltpu
from jax.sharding import PartitionSpec as P

MESH = pl.DeviceIdType.MESH
F32 = jnp.float32
BF16 = jnp.bfloat16
TILE = 128
BINS = 256
QUARTER = 64
HALO_DEV = 32
log_inner = -2.302585092994046


def halves(v):
    high = v.astype(BF16).astype(F32)
    return high, v - high


def iota(shape, dim):
    return lax.broadcasted_iota(jnp.int32, shape, dim)


def nt(a, b):
    return lax.dot_general(a, b, (((1,), (1,)), ((), ())), preferred_element_type=F32)


def bin_piece(k, bin_ref, fld_ref):
    label = jnp.concatenate([bin_ref[pl.ds(2 * k, 1), :], bin_ref[pl.ds(2 * k + 1, 1), :]], axis=1)
    low = label & (QUARTER - 1)
    high = lax.shift_right_logical(label, 6)
    v = fld_ref[:, pl.ds(pl.multiple_of(2 * TILE * k, 2 * TILE), 2 * TILE)]
    pad = jnp.zeros((1, 2 * TILE), F32)
    v8 = jnp.concatenate([v, pad, v, pad], axis=0)
    row = iota((8, 2 * TILE), 0)
    quarters = [2 * t + lax.shift_right_logical(row, 2) for t in range(2)]
    lhs = jnp.concatenate([jnp.where(high == q, part, 0.0) for part in halves(v8) for q in quarters], axis=0)
    bases = [jnp.sum(jnp.where(high < q, v8, 0.0), axis=1, keepdims=True) for q in quarters]
    below = jnp.where(low <= iota((QUARTER, 2 * TILE), 0), 1.0, 0.0).astype(BF16)
    below = jnp.concatenate([below, below], axis=0)
    out = nt(lhs.astype(BF16), below)
    return out[0:16] + out[16:32] + jnp.concatenate(bases, axis=0)


def kernel(na, nj, ny, halo_hbm, owner_hbm, bin_hbm, fld_hbm, sums, halo_ref, owner_ref, bin_ref, fld_ref,
           pieces, code_v, code_s, send_first, recv_first, send_rest, recv_rest, dense, got, in_sem, code_sem, send1, recv1, send2, recv2, ready1, ready2):
    owners = na * nj
    count = owners // 2
    pairs = na // 2
    group = nj * ny
    space = lax.axis_index("space")
    y = lax.axis_index("rad")
    a = space // nj
    j = space % nj
    me = j * ny + y

    chunks = min(2, count)
    size = count // chunks
    fetches = [pltpu.make_async_copy(halo_hbm, halo_ref, in_sem.at[0]),
               pltpu.make_async_copy(owner_hbm, owner_ref, in_sem.at[1])]
    for c in range(chunks):
        fetches.append(pltpu.make_async_copy(
            bin_hbm.at[2 * size * c:2 * size * (c + 1)], bin_ref.at[2 * size * c:2 * size * (c + 1)], in_sem.at[2 + 2 * c]))
        cells = slice(2 * TILE * size * c, 2 * TILE * size * (c + 1))
        fetches.append(pltpu.make_async_copy(fld_hbm.at[:, cells], fld_ref.at[:, cells], in_sem.at[3 + 2 * c]))
    for fetch in fetches:
        fetch.start()

    barrier = pltpu.get_barrier_semaphore()
    core = lax.rem(space, 2)
    sibling = space + 1 - 2 * core
    for turn in (2, 1, 3, 0) if nj == 16 else (0,):
        for b in range(2 if nj == 16 else 1):
            dj = lax.rem(j // 2 + turn, 4) * 2 + 8 * b if nj == 16 else 0
            for turn_y in (2, 1, 3, 0):
                dy = lax.rem(y + turn_y, ny)
                if turn or turn_y:
                    pl.semaphore_signal(barrier, inc=1, device_id=(a * nj + dj, dy), device_id_type=MESH)
                else:
                    @pl.when(dj != j)
                    def _():
                        pl.semaphore_signal(barrier, inc=1, device_id=(a * nj + dj, dy), device_id_type=MESH)
    for i in range(1, na):
        t = lax.rem(a + i, na)
        pl.semaphore_signal(barrier, inc=1, device_id=(t * nj + j // 2 * 2 + 1, y), device_id_type=MESH)

    lane = iota((8, owners), 1)

    def note(k, codes):
        halo = halo_ref[2 * k]
        code = HALO_DEV * k + (halo & (HALO_DEV - 1))
        return jnp.where(lane == owner_ref[halo], code, codes)

    def piece_and_notes(k, codes):
        pieces[k] = bin_piece(k, bin_ref, fld_ref)
        return note(2 * k + 1, note(2 * k, codes))

    def one_piece(k, carry):
        pieces[k] = bin_piece(k, bin_ref, fld_ref)
        return carry

    noting = pltpu.make_async_copy(code_v, code_s, code_sem)
    fetches[0].wait()
    fetches[1].wait()
    codes = jnp.full((8, owners), HALO_DEV * count, jnp.int32)
    pieces[count] = jnp.zeros((16, 128), F32)
    for c in range(chunks):
        fetches[2 + 2 * c].wait()
        fetches[3 + 2 * c].wait()
        if 2 * c < chunks:
            codes = lax.fori_loop(size * c, size * (c + 1), piece_and_notes, codes, unroll=size)
            if 2 * (c + 1) == chunks:
                code_v[...] = codes
                noting.start()
        else:
            lax.fori_loop(size * c, size * (c + 1), one_piece, 0, unroll=size)
    noting.wait()

    @pl.when(core == 0)
    def _():
        pl.semaphore_wait(barrier, group - 1)
        pl.semaphore_signal(ready1, inc=1, device_id=(sibling, y), device_id_type=MESH)

    @pl.when(core == 1)
    def _():
        pl.semaphore_wait(ready1, 1)

    left = iota((16, 128), 1) < QUARTER
    tagged = (iota((16, 128), 0) & 3) == 3
    block = lax.shift_right_logical(iota((8, 128), 1), 4)
    send = [send_first] + [send_rest.at[c] for c in range(pairs - 1)]
    recv = [recv_first] + [recv_rest.at[c] for c in range(pairs - 1)]

    def outbound(c, dj, dy):
        t = dj * ny + dy
        return pltpu.make_async_remote_copy(
            src_ref=send[c].at[t], dst_ref=recv[c].at[me], send_sem=send1.at[c], recv_sem=recv1.at[c],
            device_id=(a * nj + dj, dy), device_id_type=MESH)

    def everyone(c):
        return pltpu.make_async_remote_copy(
            src_ref=send[c].at[pl.ds(0, group - 1)], dst_ref=recv[c].at[pl.ds(0, group - 1)],
            send_sem=send1.at[c], recv_sem=recv1.at[c], device_id=(space, y), device_id_type=MESH)

    def onward(t, slot):
        return pltpu.make_async_remote_copy(
            src_ref=dense.at[t], dst_ref=got.at[slot], send_sem=send2.at[t], recv_sem=recv2.at[slot],
            device_id=(t * nj + j, y), device_id_type=MESH)

    turned = [2 * (p + 1 - 2 * (p % 2)) if nj == 16 and 2 * p >= pairs else 2 * p for p in range(pairs)]
    orders = [[(2 * p, 2 * p + 1) for p in range(pairs)], [(p, p + 1) for p in turned]]

    def dispatch(c):
        for turn in (2, 1, 3, 0) if nj == 16 else range(nj):
            if nj == 16:
                dests = [lax.rem(j // 2 + turn, 4) * 2 + 8 * (k % 2) + k // 2 for k in range(4)]
            else:
                dests = [lax.rem(j + turn, nj)]
            for k, dj in enumerate(dests):
                order = orders[k // 2]
                codes = [code_s[0, t * nj + dj] for t in order[c]]
                held = [pieces[lax.shift_right_logical(code, 5)] for code in codes]
                both = jnp.where(left, held[0], held[1])
                if c == 0:
                    ranks = jnp.zeros((8, 128), jnp.int32)
                    for n, t in enumerate(sum(order, ())):
                        rank = code_s[0, t * nj + dj] & (HALO_DEV - 1)
                        ranks = jnp.where(block == n, rank, ranks)
                    ranks = ranks.astype(F32)
                    both = jnp.where(tagged, jnp.concatenate([ranks, ranks], axis=0), both)
                for q in range(ny):
                    send[c][dj * ny + q] = both[4 * q:4 * q + (3 if c else 4)]
            for dj in dests:
                for turn_y in (2, 1, 3, 0):
                    dy = lax.rem(y + turn_y, ny)
                    if turn or turn_y:
                        outbound(c, dj, dy).start()
                    else:
                        @pl.when(dj != j)
                        def _():
                            outbound(c, dj, dy).start()
        recv[c][me] = send[c][me]

    for c in range(pairs):
        dispatch(c)

    @pl.when(core == 1)
    def _():
        pl.semaphore_wait(barrier, 2 * (na - 1))
        pl.semaphore_signal(ready2, inc=1, device_id=(sibling, y), device_id_type=MESH)

    for c in range(pairs):
        targets = [orders[0][c][par] + core * (orders[1][c][par] - orders[0][c][par]) for par in range(2)]
        everyone(c).wait_recv()
        if c == 0:
            labels = recv_first[:, 3, :]
            wanted = lax.rem(iota((group, 128), 1), 16)
            chosen = [jnp.where(labels == (wanted + 16 * half).astype(F32), 1.0, 0.0).T.astype(BF16) for half in range(2)]
        lhs = jnp.concatenate([rows[32 * c:32 * (c + 1)] for rows in chosen], axis=0)
        columns = [halves(recv[c][:, f, :]) for f in range(3)]
        total = sum(
            jnp.dot(lhs, jnp.concatenate([column[s] for column in columns], axis=1).astype(BF16), preferred_element_type=F32)
            for s in range(2))
        for par, t in enumerate(targets):
            for f in range(3):
                top = total[16 * par:16 * par + 16, 128 * f:128 * f + 128]
                bottom = total[16 * par + 32:16 * par + 48, 128 * f:128 * f + 128]
                if par == 0:
                    merged = jnp.where(left, top, pltpu.roll(bottom, QUARTER, 1))
                else:
                    merged = jnp.where(left, pltpu.roll(top, QUARTER, 1), bottom)
                dense[t, :, 128 * f:128 * f + 128] = merged
            if c == 0 and par == 0:
                @pl.when(core == 0)
                def _():
                    pl.semaphore_wait(ready2, 1)

            @pl.when(t != a)
            def _():
                onward(t, a).start()

    for c in range(pairs):
        everyone(c).wait_send()
    for i in range(1, na):
        t = lax.rem(a + i, na)
        onward(t, t).wait_send()
    total = dense[a]
    for i in range(1, na):
        t = lax.rem(a + i, na)
        onward(t, t).wait_recv()
        total = total + got[t]
    sums[...] = total


def finish(sums_ref, mass_ref, vol_ref, ent_ref, vel_ref):
    total = sums_ref[...]
    bins = (lax.axis_index("rad") * QUARTER + 1 + iota((16, QUARTER), 1)).astype(F32)
    radius = jnp.exp(log_inner + bins * (-log_inner / BINS))
    for f, ref in enumerate((mass_ref, vol_ref, ent_ref)):
        block = total[:, 128 * f:128 * f + 128]
        for half, part in enumerate((block, pltpu.roll(block, QUARTER, 1))):
            part = part[:, :QUARTER]
            ref[16 * half:16 * half + 16, :] = part
            if f == 0:
                vel_ref[16 * half:16 * half + 16, :] = jnp.sqrt(part / radius)


def solution(mesh):
    spaces, ny = mesh.shape["space"], mesh.shape["rad"]
    na = 8 if spaces == 128 else 2
    nj = spaces // na
    group, pairs = nj * ny, na // 2

    def body(cell_bin, cell_fields, tile_halo, halo_owner):
        vmem = pl.BlockSpec(memory_space=pltpu.VMEM)
        anywhere = pl.BlockSpec(memory_space=pl.ANY)
        dma = pltpu.SemaphoreType.DMA
        out = jax.ShapeDtypeStruct((HALO_DEV, QUARTER), F32)
        sums = pl.pallas_call(
            functools.partial(kernel, na, nj, ny),
            out_shape=pltpu.VMEM((16, 384), F32),
            in_specs=[anywhere] * 4,
            out_specs=vmem,
            scratch_shapes=[
                pltpu.SMEM(tile_halo.shape, jnp.int32),
                pltpu.SMEM(halo_owner.shape, jnp.int32),
                pltpu.VMEM((tile_halo.shape[0], TILE), jnp.int32),
                pltpu.VMEM(cell_fields.shape, F32),
                pltpu.VMEM((spaces // 2 + 1, 16, 128), F32),
                pltpu.VMEM((8, spaces), jnp.int32),
                pltpu.SMEM((8, spaces), jnp.int32),
                pltpu.VMEM((group, 4, 128), F32),
                pltpu.VMEM((group, 4, 128), F32),
                pltpu.VMEM((max(pairs - 1, 1), group, 3, 128), F32),
                pltpu.VMEM((max(pairs - 1, 1), group, 3, 128), F32),
                pltpu.VMEM((na, 16, 384), F32),
                pltpu.VMEM((na, 16, 384), F32),
                dma((10,)), dma, dma((pairs,)), dma((pairs,)), dma((na,)), dma((na,)),
                pltpu.SemaphoreType.REGULAR, pltpu.SemaphoreType.REGULAR,
            ],
            compiler_params=pltpu.CompilerParams(collective_id=0, has_side_effects=True),
            name="profiles",
        )(tile_halo, halo_owner, cell_bin.reshape(-1, TILE), cell_fields)
        return pl.pallas_call(
            finish, out_shape=(out,) * 4, in_specs=[vmem], out_specs=(vmem,) * 4, name="finish",
        )(pltpu.with_memory_space_constraint(sums, pltpu.VMEM))

    in_specs = (P(("space", "rad")), P(None, ("space", "rad")), P(("space", "rad")), P())
    out_specs = (P("space", "rad"),) * 4
    return jax.shard_map(body, mesh=mesh, in_specs=in_specs, out_specs=out_specs, check_vma=False)
```

```python
import functools

import jax
import jax.numpy as jnp
from jax import lax
from jax.experimental import pallas as pl
from jax.experimental.pallas import tpu as pltpu
from jax.sharding import PartitionSpec as P

MESH = pl.DeviceIdType.MESH
F32 = jnp.float32
BF16 = jnp.bfloat16
TILE = 128
BINS = 256
QUARTER = 64
HALO_DEV = 32
log_inner = -2.302585092994046


def halves(v):
    high = v.astype(BF16).astype(F32)
    return high, v - high


def iota(shape, dim):
    return lax.broadcasted_iota(jnp.int32, shape, dim)


def nt(a, b):
    return lax.dot_general(a, b, (((1,), (1,)), ((), ())), preferred_element_type=F32)


def bin_piece(k, bin_ref, fld_ref):
    label = jnp.concatenate([bin_ref[pl.ds(2 * k, 1), :], bin_ref[pl.ds(2 * k + 1, 1), :]], axis=1)
    low = label & (QUARTER - 1)
    high = lax.shift_right_logical(label, 6)
    v = fld_ref[:, pl.ds(pl.multiple_of(2 * TILE * k, 2 * TILE), 2 * TILE)]
    pad = jnp.zeros((1, 2 * TILE), F32)
    v8 = jnp.concatenate([v, pad, v, pad], axis=0)
    row = iota((8, 2 * TILE), 0)
    quarters = [2 * t + lax.shift_right_logical(row, 2) for t in range(2)]
    lhs = jnp.concatenate([jnp.where(high == q, part, 0.0) for part in halves(v8) for q in quarters], axis=0)
    bases = [jnp.sum(jnp.where(high < q, v8, 0.0), axis=1, keepdims=True) for q in quarters]
    below = jnp.where(low <= iota((QUARTER, 2 * TILE), 0), 1.0, 0.0).astype(BF16)
    below = jnp.concatenate([below, below], axis=0)
    out = nt(lhs.astype(BF16), below)
    return out[0:16] + out[16:32] + jnp.concatenate(bases, axis=0)


def kernel(na, nj, ny, halo_hbm, owner_hbm, bin_hbm, fld_hbm, sums, halo_ref, owner_ref, bin_ref, fld_ref,
           pieces, code_v, code_s, send_first, recv_first, send_rest, recv_rest, dense, got, in_sem, code_sem, send1, recv1, send2, recv2, ready1, ready2):
    owners = na * nj
    count = owners // 2
    pairs = na // 2
    group = nj * ny
    space = lax.axis_index("space")
    y = lax.axis_index("rad")
    a = space // nj
    j = space % nj
    me = j * ny + y

    chunks = min(2, count)
    size = count // chunks
    fetches = [pltpu.make_async_copy(halo_hbm, halo_ref, in_sem.at[0]),
               pltpu.make_async_copy(owner_hbm, owner_ref, in_sem.at[1])]
    for c in range(chunks):
        fetches.append(pltpu.make_async_copy(
            bin_hbm.at[2 * size * c:2 * size * (c + 1)], bin_ref.at[2 * size * c:2 * size * (c + 1)], in_sem.at[2 + 2 * c]))
        cells = slice(2 * TILE * size * c, 2 * TILE * size * (c + 1))
        fetches.append(pltpu.make_async_copy(fld_hbm.at[:, cells], fld_ref.at[:, cells], in_sem.at[3 + 2 * c]))
    for fetch in fetches:
        fetch.start()

    barrier = pltpu.get_barrier_semaphore()
    core = lax.rem(space, 2)
    sibling = space + 1 - 2 * core
    for turn in (2, 1, 3, 0) if nj == 16 else (0,):
        for b in range(2 if nj == 16 else 1):
            dj = lax.rem(j // 2 + turn, 4) * 2 + 8 * b if nj == 16 else 0
            for turn_y in (2, 1, 3, 0):
                dy = lax.rem(y + turn_y, ny)
                if turn or turn_y:
                    pl.semaphore_signal(barrier, inc=1, device_id=(a * nj + dj, dy), device_id_type=MESH)
                else:
                    @pl.when(dj != j)
                    def _():
                        pl.semaphore_signal(barrier, inc=1, device_id=(a * nj + dj, dy), device_id_type=MESH)
    for i in range(1, na):
        t = lax.rem(a + i, na)
        pl.semaphore_signal(barrier, inc=1, device_id=(t * nj + j // 2 * 2 + 1, y), device_id_type=MESH)

    lane = iota((8, owners), 1)

    def note(k, codes):
        halo = halo_ref[2 * k]
        code = HALO_DEV * k + (halo & (HALO_DEV - 1))
        return jnp.where(lane == owner_ref[halo], code, codes)

    def piece_and_notes(k, codes):
        pieces[k] = bin_piece(k, bin_ref, fld_ref)
        return note(2 * k + 1, note(2 * k, codes))

    def one_piece(k, carry):
        pieces[k] = bin_piece(k, bin_ref, fld_ref)
        return carry

    noting = pltpu.make_async_copy(code_v, code_s, code_sem)
    fetches[0].wait()
    fetches[1].wait()
    codes = jnp.full((8, owners), HALO_DEV * count, jnp.int32)
    pieces[count] = jnp.zeros((16, 128), F32)
    for c in range(chunks):
        fetches[2 + 2 * c].wait()
        fetches[3 + 2 * c].wait()
        if 2 * c < chunks:
            codes = lax.fori_loop(size * c, size * (c + 1), piece_and_notes, codes, unroll=size)
            if 2 * (c + 1) == chunks:
                code_v[...] = codes
                noting.start()
        else:
            lax.fori_loop(size * c, size * (c + 1), one_piece, 0, unroll=size)
    noting.wait()

    @pl.when(core == 0)
    def _():
        pl.semaphore_wait(barrier, group - 1)
        pl.semaphore_signal(ready1, inc=1, device_id=(sibling, y), device_id_type=MESH)

    @pl.when(core == 1)
    def _():
        pl.semaphore_wait(ready1, 1)

    left = iota((16, 128), 1) < QUARTER
    tagged = (iota((16, 128), 0) & 3) == 3
    block = lax.shift_right_logical(iota((8, 128), 1), 4)
    send = [send_first] + [send_rest.at[c] for c in range(pairs - 1)]
    recv = [recv_first] + [recv_rest.at[c] for c in range(pairs - 1)]

    def outbound(c, dj, dy):
        t = dj * ny + dy
        return pltpu.make_async_remote_copy(
            src_ref=send[c].at[t], dst_ref=recv[c].at[me], send_sem=send1.at[c], recv_sem=recv1.at[c],
            device_id=(a * nj + dj, dy), device_id_type=MESH)

    def everyone(c):
        return pltpu.make_async_remote_copy(
            src_ref=send[c].at[pl.ds(0, group - 1)], dst_ref=recv[c].at[pl.ds(0, group - 1)],
            send_sem=send1.at[c], recv_sem=recv1.at[c], device_id=(space, y), device_id_type=MESH)

    def onward(t, slot):
        return pltpu.make_async_remote_copy(
            src_ref=dense.at[t], dst_ref=got.at[slot], send_sem=send2.at[t], recv_sem=recv2.at[slot],
            device_id=(t * nj + j, y), device_id_type=MESH)

    turned = [2 * (p + 1 - 2 * (p % 2)) if nj == 16 and 2 * p >= pairs else 2 * p for p in range(pairs)]
    orders = [[(2 * p, 2 * p + 1) for p in range(pairs)], [(p, p + 1) for p in turned]]

    def dispatch(c):
        for turn in (2, 1, 3, 0) if nj == 16 else range(nj):
            if nj == 16:
                dests = [lax.rem(j // 2 + turn, 4) * 2 + 8 * (k % 2) + k // 2 for k in range(4)]
            else:
                dests = [lax.rem(j + turn, nj)]
            for k, dj in enumerate(dests):
                order = orders[k // 2]
                codes = [code_s[0, t * nj + dj] for t in order[c]]
                held = [pieces[lax.shift_right_logical(code, 5)] for code in codes]
                both = jnp.where(left, held[0], held[1])
                if c == 0:
                    ranks = jnp.zeros((8, 128), jnp.int32)
                    for n, t in enumerate(sum(order, ())):
                        rank = code_s[0, t * nj + dj] & (HALO_DEV - 1)
                        ranks = jnp.where(block == n, rank, ranks)
                    ranks = ranks.astype(F32)
                    both = jnp.where(tagged, jnp.concatenate([ranks, ranks], axis=0), both)
                for q in range(ny):
                    send[c][dj * ny + q] = both[4 * q:4 * q + (3 if c else 4)]
            for dj in dests:
                for turn_y in (2, 1, 3, 0):
                    dy = lax.rem(y + turn_y, ny)
                    if turn or turn_y:
                        outbound(c, dj, dy).start()
                    else:
                        @pl.when(dj != j)
                        def _():
                            outbound(c, dj, dy).start()
        recv[c][me] = send[c][me]

    for c in range(pairs):
        dispatch(c)

    @pl.when(core == 1)
    def _():
        pl.semaphore_wait(barrier, 2 * (na - 1))
        pl.semaphore_signal(ready2, inc=1, device_id=(sibling, y), device_id_type=MESH)

    for c in range(pairs):
        targets = [orders[0][c][par] + core * (orders[1][c][par] - orders[0][c][par]) for par in range(2)]
        everyone(c).wait_recv()
        if c == 0:
            labels = recv_first[:, 3, :].T
            wanted = iota((128, group), 0) & 15
            chosen = [jnp.where(labels == (wanted + 16 * half).astype(F32), 1.0, 0.0).astype(BF16) for half in range(2)]
        lhs = jnp.concatenate([rows[32 * c:32 * (c + 1)] for rows in chosen], axis=0)
        columns = [jnp.concatenate(halves(recv[c][:, f, :]), axis=0) for f in range(3)]
        total = jnp.dot(
            jnp.concatenate([lhs, lhs], axis=1), jnp.concatenate(columns, axis=1).astype(BF16), preferred_element_type=F32)
        for par, t in enumerate(targets):
            for f in range(3):
                top = total[16 * par:16 * par + 16, 128 * f:128 * f + 128]
                bottom = total[16 * par + 32:16 * par + 48, 128 * f:128 * f + 128]
                if par == 0:
                    merged = jnp.where(left, top, pltpu.roll(bottom, QUARTER, 1))
                else:
                    merged = jnp.where(left, pltpu.roll(top, QUARTER, 1), bottom)
                dense[t, :, 128 * f:128 * f + 128] = merged
            if c == 0 and par == 0:
                @pl.when(core == 0)
                def _():
                    pl.semaphore_wait(ready2, 1)

            @pl.when(t != a)
            def _():
                onward(t, a).start()

    for c in range(pairs):
        everyone(c).wait_send()
    for i in range(1, na):
        t = lax.rem(a + i, na)
        onward(t, t).wait_send()
    total = dense[a]
    for i in range(1, na):
        t = lax.rem(a + i, na)
        onward(t, t).wait_recv()
        total = total + got[t]
    sums[...] = total


def finish(sums_ref, mass_ref, vol_ref, ent_ref, vel_ref):
    total = sums_ref[...]
    bins = (lax.axis_index("rad") * QUARTER + 1 + iota((16, QUARTER), 1)).astype(F32)
    radius = jnp.exp(log_inner + bins * (-log_inner / BINS))
    for f, ref in enumerate((mass_ref, vol_ref, ent_ref)):
        block = total[:, 128 * f:128 * f + 128]
        for half, part in enumerate((block, pltpu.roll(block, QUARTER, 1))):
            part = part[:, :QUARTER]
            ref[16 * half:16 * half + 16, :] = part
            if f == 0:
                vel_ref[16 * half:16 * half + 16, :] = jnp.sqrt(part / radius)


def solution(mesh):
    spaces, ny = mesh.shape["space"], mesh.shape["rad"]
    na = 8 if spaces == 128 else 2
    nj = spaces // na
    group, pairs = nj * ny, na // 2

    def body(cell_bin, cell_fields, tile_halo, halo_owner):
        vmem = pl.BlockSpec(memory_space=pltpu.VMEM)
        anywhere = pl.BlockSpec(memory_space=pl.ANY)
        dma = pltpu.SemaphoreType.DMA
        out = jax.ShapeDtypeStruct((HALO_DEV, QUARTER), F32)
        sums = pl.pallas_call(
            functools.partial(kernel, na, nj, ny),
            out_shape=pltpu.VMEM((16, 384), F32),
            in_specs=[anywhere] * 4,
            out_specs=vmem,
            scratch_shapes=[
                pltpu.SMEM(tile_halo.shape, jnp.int32),
                pltpu.SMEM(halo_owner.shape, jnp.int32),
                pltpu.VMEM((tile_halo.shape[0], TILE), jnp.int32),
                pltpu.VMEM(cell_fields.shape, F32),
                pltpu.VMEM((spaces // 2 + 1, 16, 128), F32),
                pltpu.VMEM((8, spaces), jnp.int32),
                pltpu.SMEM((8, spaces), jnp.int32),
                pltpu.VMEM((group, 4, 128), F32),
                pltpu.VMEM((group, 4, 128), F32),
                pltpu.VMEM((max(pairs - 1, 1), group, 3, 128), F32),
                pltpu.VMEM((max(pairs - 1, 1), group, 3, 128), F32),
                pltpu.VMEM((na, 16, 384), F32),
                pltpu.VMEM((na, 16, 384), F32),
                dma((10,)), dma, dma((pairs,)), dma((pairs,)), dma((na,)), dma((na,)),
                pltpu.SemaphoreType.REGULAR, pltpu.SemaphoreType.REGULAR,
            ],
            compiler_params=pltpu.CompilerParams(collective_id=0, has_side_effects=True),
            name="profiles",
        )(tile_halo, halo_owner, cell_bin.reshape(-1, TILE), cell_fields)
        return pl.pallas_call(
            finish, out_shape=(out,) * 4, in_specs=[vmem], out_specs=(vmem,) * 4, name="finish",
        )(pltpu.with_memory_space_constraint(sums, pltpu.VMEM))

    in_specs = (P(("space", "rad")), P(None, ("space", "rad")), P(("space", "rad")), P())
    out_specs = (P("space", "rad"),) * 4
    return jax.shard_map(body, mesh=mesh, in_specs=in_specs, out_specs=out_specs, check_vma=False)
```
